8 devices in a mesh: row: 4 (over z, y, x), col: 2 (over core).
Axes of the slice: x: 2, y: 2, z: 1, core: 2. Of those that a mesh axis runs over, the one named last changes fastest.
Arguments:
- v_panels: float32 [16384, 16384], P('row', 'col')
- t_factors: float32 [128, 128, 128], P('col')
- z_vectors: float32 [16384, 1024], P(None, ('col', 'row'))
Outputs:
- output: float32 [16384, 1024], P('row', 'col')
All inputs are finite; a program needn't handle non-finite values.
Results may differ from the reference program's by a relative error of at most 0.001.
Values sent between devices are 32-bit elements.
A program may use at most 1 GiB of HBM per device.

```python
import jax
import jax.numpy as jnp
from jax import lax

MAT_ORDER = 16384
PANEL_WIDTH = 128
ROW_DEVS = 4
COL_DEVS = 2
COLS_DEV = 128
NUM_PANELS = MAT_ORDER // PANEL_WIDTH
NUM_COLS = COLS_DEV * ROW_DEVS * COL_DEVS
HIGHEST = lax.Precision.HIGHEST


def compact_factors(panels):
    gram_mat = jnp.einsum('nja,njc->jac', panels, panels, precision=HIGHEST)
    diag_half = 0.5 * gram_mat * jnp.eye(PANEL_WIDTH, dtype=jnp.float32)
    upper_mat = jnp.triu(gram_mat, 1) + diag_half
    return jnp.triu(jnp.linalg.inv(upper_mat))


def to_stored(v_log):
    rows_perm = v_log.reshape(NUM_PANELS // ROW_DEVS, ROW_DEVS, PANEL_WIDTH, MAT_ORDER)
    rows_perm = rows_perm.transpose(1, 0, 2, 3).reshape(MAT_ORDER, NUM_PANELS // COL_DEVS, COL_DEVS, PANEL_WIDTH)
    return rows_perm.transpose(0, 2, 1, 3).reshape(MAT_ORDER, MAT_ORDER)


def setup_inputs(seed: int = 0) -> dict:
    root_key = jax.random.key(seed)
    key_v, key_z = jax.random.split(root_key)
    below_diag = jax.random.normal(key_v, (MAT_ORDER, MAT_ORDER), jnp.float32)
    v_log = jnp.tril(below_diag, -1) + jnp.eye(MAT_ORDER, dtype=jnp.float32)
    t_log = compact_factors(v_log.reshape(MAT_ORDER, NUM_PANELS, PANEL_WIDTH))
    t_st = t_log.reshape(NUM_PANELS // COL_DEVS, COL_DEVS, PANEL_WIDTH, PANEL_WIDTH)
    t_st = t_st.transpose(1, 0, 2, 3).reshape(NUM_PANELS, PANEL_WIDTH, PANEL_WIDTH)
    z_draw = jax.random.normal(key_z, (MAT_ORDER, NUM_COLS), jnp.float32)
    return {'v_panels': to_stored(v_log), 't_factors': t_st, 'z_vectors': z_draw}


def reference(v_panels, t_factors, z_vectors):
    panels = v_panels.reshape(MAT_ORDER, COL_DEVS, NUM_PANELS // COL_DEVS, PANEL_WIDTH)
    panels = panels.transpose(2, 1, 0, 3).reshape(NUM_PANELS, MAT_ORDER, PANEL_WIDTH)
    factors = t_factors.reshape(COL_DEVS, NUM_PANELS // COL_DEVS, PANEL_WIDTH, PANEL_WIDTH)
    factors = factors.transpose(1, 0, 2, 3).reshape(NUM_PANELS, PANEL_WIDTH, PANEL_WIDTH)

    def apply_panel(x_cur, panel_item):
        v_j, t_j = panel_item
        w_mat = jnp.dot(v_j.T, x_cur, precision=HIGHEST, preferred_element_type=jnp.float32)
        y_mat = jnp.dot(t_j, w_mat, precision=HIGHEST, preferred_element_type=jnp.float32)
        x_new = x_cur - jnp.dot(v_j, y_mat, precision=HIGHEST, preferred_element_type=jnp.float32)
        return x_new, None

    return lax.scan(apply_panel, z_vectors, (panels, factors), reverse=True)[0]
```

```python
import functools

import jax
import jax.numpy as jnp
from jax import lax
from jax.experimental import pallas as pl
from jax.experimental.pallas import tpu as pltpu
from jax.sharding import PartitionSpec as P

HIGHEST = lax.Precision.HIGHEST
F32 = jnp.float32
BF16 = jnp.bfloat16
MESH = pl.DeviceIdType.MESH
NN = (((1,), (0,)), ((), ()))
NT = (((1,), (1,)), ((), ()))
C = 128
B = 256
SH = 32


def dg(a, b, dims):
    return lax.dot_general(a, b, dims, preferred_element_type=F32)


def split3(x):
    x0 = x.astype(BF16)
    r1 = x - x0.astype(F32)
    x1 = r1.astype(BF16)
    x2 = (r1 - x1.astype(F32)).astype(BF16)
    return x0, x1, x2


def kernel(R, NB, t_hbm, v_hbm, z_hbm, out_hbm,
           xT, vst, vb, tb, ysp, xs, wacc, wsend, wrecv, ysend, yT,
           z_send, z_recv, z_loc, v_send, v_recv, v_loc, t_sem,
           rs_send, rs_recv, ag_send, ag_recv, o_sem, vfree):
    NL = xT.shape[1]
    NT_TILES = NL // R
    TB = R // 64
    me = lax.axis_index('row')
    e = lax.axis_index('col')
    px, py = lax.rem(me, 2), me // 2
    peers = [py * 2 + (1 - px), (1 - py) * 2 + px, 3 - me]

    def rows_of(t):
        return pl.ds(pl.multiple_of(t * R, R), R)

    def lo_v(q):
        return jnp.maximum(q - 1, 0) // TB

    def z_remote(t, p):
        return pltpu.make_async_remote_copy(
            src_ref=z_hbm.at[:, pl.ds(pl.multiple_of(peers[p] * NL + t * R, R), R)],
            dst_ref=xT.at[pl.ds(pl.multiple_of(me * C, C), C), rows_of(t)],
            send_sem=z_send.at[t, p], recv_sem=z_recv.at[t, p],
            device_id=(peers[p], e), device_id_type=MESH)

    def z_local(t):
        return pltpu.make_async_copy(
            z_hbm.at[:, pl.ds(pl.multiple_of(me * NL + t * R, R), R)],
            xT.at[pl.ds(pl.multiple_of(me * C, C), C), rows_of(t)], z_loc.at[t])

    def v_remote(q, t):
        s = lax.rem(q, 2)
        return pltpu.make_async_remote_copy(
            src_ref=v_hbm.at[rows_of(t), pl.ds(pl.multiple_of(q * 128, 128), 128)],
            dst_ref=vst.at[s, e, rows_of(t), :],
            send_sem=v_send.at[s, t], recv_sem=v_recv.at[s, t],
            device_id=(me, 1 - e), device_id_type=MESH)

    def v_local(q, t):
        s = lax.rem(q, 2)
        return pltpu.make_async_copy(
            v_hbm.at[rows_of(t), pl.ds(pl.multiple_of(q * 128, 128), 128)],
            vst.at[s, e, rows_of(t), :], v_loc.at[s, t])

    def t_copy(q):
        return pltpu.make_async_copy(t_hbm.at[q], tb.at[lax.rem(q, 2)], t_sem.at[lax.rem(q, 2)])

    def rs_copy(c, p):
        return pltpu.make_async_remote_copy(
            src_ref=wsend.at[c, pl.ds(pl.multiple_of(peers[p] * SH, SH), SH), :],
            dst_ref=wrecv.at[c, p], send_sem=rs_send.at[c, p], recv_sem=rs_recv.at[c, p],
            device_id=(peers[p], e), device_id_type=MESH)

    def ag_copy(c, p):
        return pltpu.make_async_remote_copy(
            src_ref=ysend.at[c],
            dst_ref=yT.at[c, pl.ds(pl.multiple_of(me * SH, SH), SH), :],
            send_sem=ag_send.at[c, p], recv_sem=ag_recv.at[c, p],
            device_id=(peers[p], e), device_id_type=MESH)

    def v_fetch(q):
        def one(t, _):
            v_remote(q, t).start()
            v_local(q, t).start()
            return 0
        lax.fori_loop(lo_v(q), NT_TILES, one, 0)

    def v_sent(q):
        def one(t, _):
            v_remote(q, t).wait_send()
            return 0
        lax.fori_loop(lo_v(q), NT_TILES, one, 0)

    def prep_tile(q, t):
        s = lax.rem(q, 2)
        s3 = lax.rem(q, 3)
        v_local(q, t).wait()
        v_remote(q, t).wait_recv()
        rows = rows_of(t)
        for h in range(2):
            pieces = split3(vst[s, h, rows, :])
            for k in range(3):
                vb[s3, k, rows, h * 128:(h + 1) * 128] = pieces[k]

    def upd_tile(b, c, t, k):
        s3 = lax.rem(b, 3)
        rows = rows_of(t)
        cs = pl.ds(pl.multiple_of(c * C, C), C)
        p = dg(ysp[...], vb[s3, 0, rows, :], NT)
        q = dg(ysp[0:2 * C, :], vb[s3, 1, rows, :], NT)
        r = dg(ysp[0:C, :], vb[s3, 2, rows, :], NT)
        x = xT[cs, rows] - (p[0:C] + (p[C:2 * C] + q[0:C]) + (p[2 * C:] + q[C:] + r))
        xT[cs, rows] = x
        if k is not None:
            for i, piece in enumerate(split3(x)):
                xs[k, i * C:(i + 1) * C, :] = piece

    def w_tile(q, t, k):
        s3 = lax.rem(q, 3)
        rows = rows_of(t)
        p = dg(xs[k], vb[s3, 0, rows, :], NN)
        u = dg(xs[k, 0:2 * C], vb[s3, 1, rows, :], NN)
        r = dg(xs[k, 0:C], vb[s3, 2, rows, :], NN)
        wacc[...] += p[0:C] + (p[C:2 * C] + u[0:C]) + (p[2 * C:] + u[C:] + r)

    def w_send(c):
        wsend[c] = wacc[...]
        for p in range(3):
            rs_copy(c, p).start()

    def rs_handle(j):
        c = lax.rem(j, 4)
        q = NB - 1 - j // 4
        for p in range(3):
            rs_copy(c, p).wait_recv()
        mine = pl.ds(pl.multiple_of(me * SH, SH), SH)
        w = (wsend[c, mine, :] + wrecv[c, 0]) + (wrecv[c, 1] + wrecv[c, 2])
        y = lax.dot_general(w, tb[lax.rem(q, 2)], NT, precision=HIGHEST, preferred_element_type=F32)
        ysend[c] = y
        yT[c, mine, :] = y
        for p in range(3):
            ag_copy(c, p).start()

    def ag_wait(c):
        for p in range(3):
            ag_copy(c, p).wait_recv()
        for i, piece in enumerate(split3(yT[c])):
            ysp[i * C:(i + 1) * C, :] = piece

    def z_wait(t):
        z_local(t).wait()
        for p in range(3):
            z_remote(t, p).wait_recv()

    barrier = pltpu.get_barrier_semaphore()
    for p in range(3):
        pl.semaphore_signal(barrier, inc=1, device_id=(peers[p], e), device_id_type=MESH)
    pl.semaphore_signal(barrier, inc=1, device_id=(me, 1 - e), device_id_type=MESH)
    pl.semaphore_wait(barrier, 4)

    v_fetch(NB - 1)
    v_fetch(NB - 2)
    t_copy(NB - 1).start()
    t_copy(NB - 2).start()

    def z_start(n, _):
        t = NT_TILES - 1 - n
        for p in range(3):
            z_remote(t, p).start()
        z_local(t).start()
        return 0
    lax.fori_loop(0, NT_TILES, z_start, 0)

    def prep_all(q):
        def one(t, _):
            prep_tile(q, t)
            return 0
        lax.fori_loop(lo_v(q), NT_TILES, one, 0)

    def v_release(q):
        pl.semaphore_signal(vfree, inc=1, device_id=(me, 1 - e), device_id_type=MESH)
        v_sent(q)
        pl.semaphore_wait(vfree, 1)
        v_fetch(q - 2)

    prep_all(NB - 1)
    v_release(NB - 1)
    prep_all(NB - 2)
    v_release(NB - 2)

    last = NT_TILES - 1
    z_wait(last)
    t_copy(NB - 1).wait()

    def first_w(c, _):
        cs = pl.ds(pl.multiple_of(c * C, C), C)
        for i, piece in enumerate(split3(xT[cs, last * R:(last + 1) * R])):
            xs[0, i * C:(i + 1) * C, :] = piece
        wacc[...] = jnp.zeros_like(wacc)
        w_tile(NB - 1, last, 0)
        w_send(c)
        return 0
    lax.fori_loop(0, 4, first_w, 0)
    rs_handle(0)
    rs_handle(1)

    def slot(i, _):
        b = NB - 1 - i // 4
        c = lax.rem(i, 4)

        @pl.when(jnp.logical_and(c == 0, lax.rem(b, TB) == 0))
        def _():
            z_wait((b - 1) // TB)

        @pl.when(jnp.logical_and(c == 2, b >= 1))
        def _():
            t_copy(b - 1).wait()

            @pl.when(b >= 2)
            def _():
                t_copy(b - 2).start()

        for p in range(3):
            ag_copy(c, p).wait_send()
        ag_wait(c)
        wacc[...] = jnp.zeros_like(wacc)
        lo = (b - 1) // TB
        upd_tile(b, c, lo, lax.rem(lo, 2))

        def tile(t, _):
            w_tile(b - 1, t - 1, lax.rem(t - 1, 2))
            upd_tile(b, c, t, lax.rem(t, 2))
            return 0
        lax.fori_loop(lo + 1, NT_TILES, tile, 0)
        rs_handle(i + 2)
        w_tile(b - 1, last, last % 2)
        for p in range(3):
            rs_copy(c, p).wait_send()
        w_send(c)

        @pl.when(b >= 2)
        def _():
            q = b - 2
            for h in range((NT_TILES + 3) // 4):
                t = c + 4 * h

                @pl.when(jnp.logical_and(t >= lo_v(q), t < NT_TILES))
                def _():
                    prep_tile(q, t)

            @pl.when(jnp.logical_and(c == 3, q >= 2))
            def _():
                v_release(q)
        return 0

    lax.fori_loop(0, 4 * (NB - 1), slot, 0)

    def end_slot(c, _):
        for p in range(3):
            ag_copy(c, p).wait_send()
            rs_copy(c, p).wait_send()
        ag_wait(c)

        def tile(t, _):
            upd_tile(0, c, t, None)
            return 0
        lax.fori_loop(0, NT_TILES, tile, 0)
        cs = pl.ds(pl.multiple_of(c * C, C), C)
        pltpu.make_async_copy(xT.at[cs, :], out_hbm.at[cs, :], o_sem.at[c]).start()

        @pl.when(c < 2)
        def _():
            rs_handle(4 * (NB - 1) + c + 2)
        return 0
    lax.fori_loop(0, 4, end_slot, 0)

    for c in range(4):
        cs = pl.ds(c * C, C)
        pltpu.make_async_copy(xT.at[cs, :], out_hbm.at[cs, :], o_sem.at[c]).wait()

    def z_sent(t, _):
        for p in range(3):
            z_remote(t, p).wait_send()
        return 0
    lax.fori_loop(0, NT_TILES, z_sent, 0)
    v_sent(1)
    v_sent(0)


def solution(mesh):
    def local_apply(v_loc, t_loc, z_loc):
        NL, half = v_loc.shape
        NB = half // 128
        R = min(512, NL // 4)
        tiles = NL // R
        e = lax.axis_index('col')
        other = lax.ppermute(v_loc, 'col', [(0, 1), (1, 0)])
        v0 = jnp.where(e == 0, v_loc, other).reshape(NL, NB, 128)
        v1 = jnp.where(e == 0, other, v_loc).reshape(NL, NB, 128)
        gram = lax.psum(jnp.einsum('rla,rlb->lab', v0, v1, precision=HIGHEST), 'row')
        t_all = lax.all_gather(t_loc, 'col', axis=0)
        t01 = -jnp.einsum('lab,lbc,lcd->lad', t_all[0], gram, t_all[1], precision=HIGHEST)
        t_pair = jnp.concatenate([
            jnp.concatenate([t_all[0], t01], axis=2),
            jnp.concatenate([jnp.zeros_like(t01), t_all[1]], axis=2)], axis=1)
        z_t = z_loc.T
        any_ = pl.BlockSpec(memory_space=pl.ANY)
        dma = pltpu.SemaphoreType.DMA
        x_t = pl.pallas_call(
            functools.partial(kernel, R, NB),
            out_shape=jax.ShapeDtypeStruct((4 * C, NL), F32),
            in_specs=[any_] * 3,
            out_specs=any_,
            scratch_shapes=[
                pltpu.VMEM((4 * C, NL), F32),
                pltpu.VMEM((2, 2, NL, 128), F32),
                pltpu.VMEM((3, 3, NL, B), BF16),
                pltpu.VMEM((2, B, B), F32),
                pltpu.VMEM((3 * C, B), BF16),
                pltpu.VMEM((2, 3 * C, R), BF16),
                pltpu.VMEM((C, B), F32),
                pltpu.VMEM((4, C, B), F32),
                pltpu.VMEM((4, 3, SH, B), F32),
                pltpu.VMEM((4, SH, B), F32),
                pltpu.VMEM((4, C, B), F32),
                dma((tiles, 3)), dma((tiles, 3)), dma((tiles,)),
                dma((2, tiles)), dma((2, tiles)), dma((2, tiles)), dma((2,)),
                dma((4, 3)), dma((4, 3)), dma((4, 3)), dma((4, 3)), dma((4,)),
                pltpu.SemaphoreType.REGULAR,
            ],
            compiler_params=pltpu.CompilerParams(
                collective_id=0, has_side_effects=True, vmem_limit_bytes=62 * 1024 * 1024),
            name='back_transform',
        )(t_pair, v_loc, z_t)
        return x_t.T

    return jax.shard_map(local_apply, mesh=mesh,
                         in_specs=(P('row', 'col'), P('col', None, None), P(None, ('col', 'row'))),
                         out_specs=P('row', 'col'), check_vma=False)
```

```python
import functools

import jax
import jax.numpy as jnp
from jax import lax
from jax.experimental import pallas as pl
from jax.experimental.pallas import tpu as pltpu
from jax.sharding import PartitionSpec as P

HIGHEST = lax.Precision.HIGHEST
F32 = jnp.float32
BF16 = jnp.bfloat16
MESH = pl.DeviceIdType.MESH
NN = (((1,), (0,)), ((), ()))
NT = (((1,), (1,)), ((), ()))
C = 128
B = 256
SH = 32


def dg(a, b, dims=NN):
    return lax.dot_general(a, b, dims, preferred_element_type=F32)


def split3(x):
    x0 = x.astype(BF16)
    r1 = x - x0.astype(F32)
    x1 = r1.astype(BF16)
    x2 = (r1 - x1.astype(F32)).astype(BF16)
    return x0, x1, x2


def dot6(m, stack, b0, b1, b2, dims=NN):
    p = dg(stack[0:3 * m], b0, dims)
    q = dg(stack[0:2 * m], b1, dims)
    r = dg(stack[0:m], b2, dims)
    return p[0:m] + (p[m:2 * m] + q[0:m]) + (p[2 * m:] + q[m:] + r)


def kernel(R, NB, t_hbm, v_hbm, z_hbm, out_hbm,
           xT, vst, vb, tst, tp, ysp, xsa, xsb, wacc, wsend, wrecv, ysend, yT,
           gacc, gsend, grecv, gown, gfull, t01s, t01r,
           z_send, z_recv, z_loc, v_send, v_recv, v_loc, t_send, t_recv, t_loc,
           rs_send, rs_recv, ag_send, ag_recv, g_sems, p_send, p_recv, o_sem, vfree):
    NL = xT.shape[1]
    NTL = NL // R
    TB = R // 64
    H = R // 2
    G = R // 4
    ZP = R // 128
    me = lax.axis_index('row')
    e = lax.axis_index('col')
    px, py = lax.rem(me, 2), me // 2
    peers = [py * 2 + (1 - px), (1 - py) * 2 + px, 3 - me]
    mine = pl.ds(pl.multiple_of(me * SH, SH), SH)

    def rows_of(t):
        return pl.ds(pl.multiple_of(t * R, R), R)

    def chunk(c):
        return pl.ds(pl.multiple_of(c * C, C), C)

    def lo_v(q):
        return jnp.maximum(q - 1, 0) // TB

    def own(q):
        return lax.rem(q, 2) == e

    def z_remote(k, p):
        return pltpu.make_async_remote_copy(
            src_ref=z_hbm.at[:, pl.ds(pl.multiple_of(peers[p] * NL + k * 128, 128), 128)],
            dst_ref=xT.at[chunk(me), pl.ds(pl.multiple_of(k * 128, 128), 128)],
            send_sem=z_send.at[k, p], recv_sem=z_recv.at[k, p],
            device_id=(peers[p], e), device_id_type=MESH)

    def z_local(k):
        return pltpu.make_async_copy(
            z_hbm.at[:, pl.ds(pl.multiple_of(me * NL + k * 128, 128), 128)],
            xT.at[chunk(me), pl.ds(pl.multiple_of(k * 128, 128), 128)], z_loc.at[k])

    def v_remote(q, t):
        s = lax.rem(q, 2)
        return pltpu.make_async_remote_copy(
            src_ref=v_hbm.at[rows_of(t), pl.ds(pl.multiple_of(q * 128, 128), 128)],
            dst_ref=vst.at[s, e, rows_of(t), :],
            send_sem=v_send.at[s, t], recv_sem=v_recv.at[s, t],
            device_id=(me, 1 - e), device_id_type=MESH)

    def v_local(q, t):
        s = lax.rem(q, 2)
        return pltpu.make_async_copy(
            v_hbm.at[rows_of(t), pl.ds(pl.multiple_of(q * 128, 128), 128)],
            vst.at[s, e, rows_of(t), :], v_loc.at[s, t])

    def t_remote(q):
        s = lax.rem(q, 4)
        return pltpu.make_async_remote_copy(
            src_ref=t_hbm.at[q], dst_ref=tst.at[s, e], send_sem=t_send.at[s], recv_sem=t_recv.at[s],
            device_id=(me, 1 - e), device_id_type=MESH)

    def t_local(q):
        s = lax.rem(q, 4)
        return pltpu.make_async_copy(t_hbm.at[q], tst.at[s, e], t_loc.at[s])

    def t01_copy(q):
        s = lax.rem(q // 2, 2)
        return pltpu.make_async_remote_copy(
            src_ref=t01s.at[s], dst_ref=t01r.at[s], send_sem=p_send.at[s], recv_sem=p_recv.at[s],
            device_id=(me, 1 - e), device_id_type=MESH)

    def rs_copy(c, p):
        return pltpu.make_async_remote_copy(
            src_ref=wsend.at[c, pl.ds(pl.multiple_of(peers[p] * SH, SH), SH), :],
            dst_ref=wrecv.at[c, p], send_sem=rs_send.at[c, p], recv_sem=rs_recv.at[c, p],
            device_id=(peers[p], e), device_id_type=MESH)

    def ag_copy(c, p):
        return pltpu.make_async_remote_copy(
            src_ref=ysend.at[c], dst_ref=yT.at[c, mine, :],
            send_sem=ag_send.at[c, p], recv_sem=ag_recv.at[c, p],
            device_id=(peers[p], e), device_id_type=MESH)

    def grs_copy(p):
        return pltpu.make_async_remote_copy(
            src_ref=gsend.at[pl.ds(pl.multiple_of(peers[p] * SH, SH), SH), :],
            dst_ref=grecv.at[p], send_sem=g_sems.at[0, p], recv_sem=g_sems.at[1, p],
            device_id=(peers[p], e), device_id_type=MESH)

    def gag_copy(p):
        return pltpu.make_async_remote_copy(
            src_ref=gown, dst_ref=gfull.at[mine, :], send_sem=g_sems.at[2, p], recv_sem=g_sems.at[3, p],
            device_id=(peers[p], e), device_id_type=MESH)

    def over_tiles(q, fn):
        def one(t, _):
            fn(q, t)
            return 0
        lax.fori_loop(lo_v(q), NTL, one, 0)

    def fetch(q):
        def one(q, t):
            v_remote(q, t).start()
            v_local(q, t).start()
        over_tiles(q, one)
        t_remote(q).start()
        t_local(q).start()

    def arrived(q):
        def one(q, t):
            v_local(q, t).wait()
            v_remote(q, t).wait_recv()
        over_tiles(q, one)
        t_local(q).wait()
        t_remote(q).wait_recv()

    def sent(q):
        over_tiles(q, lambda q, t: v_remote(q, t).wait_send())
        t_remote(q).wait_send()

    def release(q):
        pl.semaphore_signal(vfree, inc=1, device_id=(me, 1 - e), device_id_type=MESH)
        sent(q)
        pl.semaphore_wait(vfree, 1)
        fetch(q - 2)

    def prep(q, r0, gram):
        s, s4 = lax.rem(q, 2), lax.rem(q, 4)
        rows = pl.ds(pl.multiple_of(r0, G), G)
        f0, f1 = vst[s, 0, rows, :], vst[s, 1, rows, :]
        p0, p1 = split3(f0), split3(f1)
        for k in range(3):
            vb[s4, k, rows, 0:128] = p0[k]
            vb[s4, k, rows, 128:256] = p1[k]
        if gram:
            gacc[...] += dot6(128, jnp.concatenate(split3(f0.T), axis=0), *p1)

    def g_start(q):
        gsend[...] = gacc[...]
        for p in range(3):
            grs_copy(p).start()

    def g_mid(q):
        for p in range(3):
            grs_copy(p).wait_recv()
        g = (gsend[mine, :] + grecv[0]) + (grecv[1] + grecv[2])
        gown[...] = g
        gfull[mine, :] = g
        for p in range(3):
            gag_copy(p).start()

    def g_fin(q):
        for p in range(3):
            gag_copy(p).wait_recv()
            grs_copy(p).wait_send()
            gag_copy(p).wait_send()
        s = lax.rem(q, 4)
        u = lax.dot_general(tst[s, 0], gfull[...], NN, precision=HIGHEST, preferred_element_type=F32)
        t01 = -lax.dot_general(u, tst[s, 1], NN, precision=HIGHEST, preferred_element_type=F32)
        t01s[lax.rem(q // 2, 2)] = t01
        t01_copy(q).start()

    def t_build(q):
        s, s2, sh = lax.rem(q, 4), lax.rem(q, 2), lax.rem(q // 2, 2)

        def put(t01):
            tt = jnp.concatenate([
                jnp.concatenate([tst[s, 0].T, jnp.zeros((128, 128), F32)], axis=1),
                jnp.concatenate([t01.T, tst[s, 1].T], axis=1)], axis=0)
            for k, piece in enumerate(split3(tt)):
                tp[s2, k] = piece

        @pl.when(own(q))
        def _():
            t01_copy(q).wait_send()
            put(t01s[sh])

        @pl.when(jnp.logical_not(own(q)))
        def _():
            t01_copy(q).wait_recv()
            put(t01r[sh])

    def upd(b, c, r0, xs):
        s4 = lax.rem(b, 4)
        rows = pl.ds(pl.multiple_of(r0, H), H)
        d = dot6(C, ysp[...], vb[s4, 0, rows, :], vb[s4, 1, rows, :], vb[s4, 2, rows, :], NT)
        x = xT[chunk(c), rows] - d
        xT[chunk(c), rows] = x
        if xs is not None:
            for i, piece in enumerate(split3(x)):
                xs[i * C:(i + 1) * C, :] = piece

    def wprod(q, r0, xs):
        s4 = lax.rem(q, 4)
        rows = pl.ds(pl.multiple_of(r0, H), H)
        return dot6(C, xs[...], vb[s4, 0, rows, :], vb[s4, 1, rows, :], vb[s4, 2, rows, :])

    def body(b, c, t, first, gram):
        lo = (b - 1) // TB
        q = jnp.maximum(b - 3, 0)
        ra = t * R
        upd(b, c, ra, xsa)
        prep(q, lo * R + (c * (NTL - lo) + (t - lo)) * G, gram)
        w = None if first else wprod(b - 1, ra - H, xsb)
        upd(b, c, ra + H, xsb)
        if first:
            wacc[...] = wprod(b - 1, ra, xsa)
        else:
            wacc[...] += w + wprod(b - 1, ra, xsa)

    def rs_wait(j):
        for p in range(3):
            rs_copy(lax.rem(j, 4), p).wait_recv()

    def rs_sum(j):
        c = lax.rem(j, 4)
        s2 = lax.rem(NB - 1 - j // 4, 2)
        w = (wsend[c, mine, :] + wrecv[c, 0]) + (wrecv[c, 1] + wrecv[c, 2])
        y = dot6(SH, jnp.concatenate(split3(w), axis=0), tp[s2, 0], tp[s2, 1], tp[s2, 2])
        ysend[c] = y
        yT[c, mine, :] = y

    def y_send(j):
        for p in range(3):
            ag_copy(lax.rem(j, 4), p).start()

    def w_send(c):
        for p in range(3):
            rs_copy(c, p).start()

    def y_take(c):
        for p in range(3):
            ag_copy(c, p).wait_recv()
            ag_copy(c, p).wait_send()
            rs_copy(c, p).wait_send()
        for i, piece in enumerate(split3(yT[c])):
            ysp[i * C:(i + 1) * C, :] = piece

    def z_start(k):
        for p in range(3):
            z_remote(k, p).start()
        z_local(k).start()

    def z_wait(t):
        def one(k, _):
            z_local(k).wait()
            for p in range(3):
                z_remote(k, p).wait_recv()
            return 0
        lax.fori_loop(t * ZP, (t + 1) * ZP, one, 0)

    barrier = pltpu.get_barrier_semaphore()
    for p in range(3):
        pl.semaphore_signal(barrier, inc=1, device_id=(peers[p], e), device_id_type=MESH)
    pl.semaphore_signal(barrier, inc=1, device_id=(me, 1 - e), device_id_type=MESH)
    pl.semaphore_wait(barrier, 4)

    fetch(NB - 1)
    fetch(NB - 2)

    def z_first(n, _):
        z_start(NTL * ZP - 1 - n)
        return 0
    lax.fori_loop(0, ZP, z_first, 0)

    def prep_all(q):
        arrived(q)

        def one(n, _):
            prep(q, lo_v(q) * R + n * G, True)
            return 0

        gacc[...] = jnp.zeros_like(gacc)
        lax.fori_loop(0, 4 * (NTL - lo_v(q)), one, 0)

    def when_own(q, fn):
        @pl.when(own(q))
        def _():
            fn(q)

    prep_all(NB - 1)
    when_own(NB - 1, g_start)
    release(NB - 1)
    prep_all(NB - 2)
    when_own(NB - 2, g_start)
    release(NB - 2)
    when_own(NB - 1, g_mid)
    when_own(NB - 2, g_mid)
    when_own(NB - 1, g_fin)
    when_own(NB - 2, g_fin)
    prep_all(NB - 3)
    when_own(NB - 3, g_start)
    t_build(NB - 1)
    release(NB - 3)
    z_wait(NTL - 1)

    def first_w(c, _):
        base = (NTL - 1) * R
        for n, xs in enumerate((xsa, xsb)):
            for i, piece in enumerate(split3(xT[chunk(c), base + n * H:base + (n + 1) * H])):
                xs[i * C:(i + 1) * C, :] = piece
        wsend[c] = wprod(NB - 1, base, xsa) + wprod(NB - 1, base + H, xsb)
        w_send(c)
        return 0
    lax.fori_loop(0, 4, first_w, 0)
    for j in range(2):
        rs_wait(j)
        rs_sum(j)
        y_send(j)

    def slot(i, _):
        b = NB - 1 - i // 4
        c = lax.rem(i, 4)
        lo = (b - 1) // TB
        q3 = b - 3

        @pl.when(c == 0)
        def _():
            @pl.when(lax.rem(b, TB) == 0)
            def _():
                z_wait(lo)

            @pl.when(jnp.logical_and(lo >= 1, lax.rem(TB * (lo + 1) - 1 - b, TB // ZP) == 0))
            def _():
                z_start((lo - 1) * ZP + ZP - 1 - (TB * (lo + 1) - 1 - b) // (TB // ZP))

            @pl.when(q3 >= 0)
            def _():
                arrived(q3)
                gacc[...] = jnp.zeros_like(gacc)

        @pl.when(c == 1)
        def _():
            @pl.when(jnp.logical_and(own(b - 2), b >= 2))
            def _():
                g_mid(b - 2)
            t_build(b - 1)

        @pl.when(jnp.logical_and(q3 >= 0, lo_v(q3) < lo))
        def _():
            @pl.when(own(q3))
            def _():
                prep(q3, lo_v(q3) * R + c * G, True)

            @pl.when(jnp.logical_not(own(q3)))
            def _():
                prep(q3, lo_v(q3) * R + c * G, False)

        def run(gram):
            y_take(c)
            body(b, c, lo, True, gram)

            def tile(t, _):
                body(b, c, t, False, gram)
                return 0
            lax.fori_loop(lo + 1, NTL, tile, 0)

        with_gram = jnp.logical_and(q3 >= 0, own(q3))

        @pl.when(with_gram)
        def _():
            run(True)

        @pl.when(jnp.logical_not(with_gram))
        def _():
            run(False)

        rs_wait(i + 2)
        rs_sum(i + 2)
        wsend[c] = wacc[...] + wprod(b - 1, NL - H, xsb)
        y_send(i + 2)
        w_send(c)

        @pl.when(c == 3)
        def _():
            @pl.when(jnp.logical_and(own(b - 2), b >= 2))
            def _():
                g_fin(b - 2)

            @pl.when(with_gram)
            def _():
                g_start(q3)

            @pl.when(q3 >= 2)
            def _():
                release(q3)
        return 0

    lax.fori_loop(0, 4 * (NB - 1), slot, 0)

    def out_copy(c):
        return pltpu.make_async_copy(xT.at[chunk(c), :], out_hbm.at[chunk(c), :], o_sem.at[c])

    def end_slot(c, _):
        @pl.when(c < 2)
        def _():
            j = 4 * (NB - 1) + c + 2
            rs_wait(j)
            rs_sum(j)
            y_send(j)
        y_take(c)

        def tile(t, _):
            upd(0, c, t * R, None)
            upd(0, c, t * R + H, None)
            return 0
        lax.fori_loop(0, NTL, tile, 0)
        out_copy(c).start()
        return 0
    lax.fori_loop(0, 4, end_slot, 0)

    for c in range(4):
        out_copy(c).wait()

    def z_sent(k, _):
        for p in range(3):
            z_remote(k, p).wait_send()
        return 0
    lax.fori_loop(0, NTL * ZP, z_sent, 0)
    sent(1)
    sent(0)


def solution(mesh):
    def local_apply(v_loc, t_loc, z_loc):
        NL, half = v_loc.shape
        NB = half // 128
        R = min(1024, NL // 2)
        tiles = NL // R
        H = R // 2
        z_t = z_loc.T
        any_ = pl.BlockSpec(memory_space=pl.ANY)
        dma = pltpu.SemaphoreType.DMA
        vmem = pltpu.VMEM
        x_t = pl.pallas_call(
            functools.partial(kernel, R, NB),
            out_shape=jax.ShapeDtypeStruct((4 * C, NL), F32),
            in_specs=[any_] * 3,
            out_specs=any_,
            scratch_shapes=[
                vmem((4 * C, NL), F32),
                vmem((2, 2, NL, 128), F32),
                vmem((4, 3, NL, B), BF16),
                vmem((4, 2, 128, 128), F32),
                vmem((2, 3, B, B), BF16),
                vmem((3 * C, B), BF16),
                vmem((3 * C, H), BF16),
                vmem((3 * C, H), BF16),
                vmem((C, B), F32),
                vmem((4, C, B), F32),
                vmem((4, 3, SH, B), F32),
                vmem((4, SH, B), F32),
                vmem((4, C, B), F32),
                vmem((128, 128), F32),
                vmem((128, 128), F32),
                vmem((3, SH, 128), F32),
                vmem((SH, 128), F32),
                vmem((128, 128), F32),
                vmem((2, 128, 128), F32),
                vmem((2, 128, 128), F32),
                dma((NL // 128, 3)), dma((NL // 128, 3)), dma((NL // 128,)),
                dma((2, tiles)), dma((2, tiles)), dma((2, tiles)),
                dma((4,)), dma((4,)), dma((4,)),
                dma((4, 3)), dma((4, 3)), dma((4, 3)), dma((4, 3)),
                dma((4, 3)), dma((2,)), dma((2,)), dma((4,)),
                pltpu.SemaphoreType.REGULAR,
            ],
            compiler_params=pltpu.CompilerParams(
                collective_id=0, has_side_effects=True, vmem_limit_bytes=62 * 1024 * 1024),
            name='back_transform',
        )(t_loc, v_loc, z_t)
        return x_t.T

    return jax.shard_map(local_apply, mesh=mesh,
                         in_specs=(P('row', 'col'), P('col', None, None), P(None, ('col', 'row'))),
                         out_specs=P('row', 'col'), check_vma=False)
```

```python
import functools

import jax
import jax.numpy as jnp
from jax import lax
from jax.experimental import pallas as pl
from jax.experimental.pallas import tpu as pltpu
from jax.sharding import PartitionSpec as P

HIGHEST = lax.Precision.HIGHEST
F32 = jnp.float32
BF16 = jnp.bfloat16
MESH = pl.DeviceIdType.MESH
NN = (((1,), (0,)), ((), ()))
NT = (((1,), (1,)), ((), ()))
C = 128
B = 256
SH = 32


def dg(a, b, dims=NN):
    return lax.dot_general(a, b, dims, preferred_element_type=F32)


def split3(x):
    x0 = x.astype(BF16)
    r1 = x - x0.astype(F32)
    x1 = r1.astype(BF16)
    x2 = (r1 - x1.astype(F32)).astype(BF16)
    return x0, x1, x2


def dot6(m, stack, b0, b1, b2, dims=NN):
    p = dg(stack[0:3 * m], b0, dims)
    q = dg(stack[0:2 * m], b1, dims)
    r = dg(stack[0:m], b2, dims)
    return p[0:m] + (p[m:2 * m] + q[0:m]) + (p[2 * m:] + q[m:] + r)


def kernel(H, NB, t_hbm, v_hbm, z_hbm, out_hbm,
           xT, vst, vb, tst, tp, ysp, xs, wacc, wsend, wrecv, ysend, yT,
           gacc, gsend, grecv, gown, gfull, t01s, t01r,
           z_send, z_recv, z_loc, v_send, v_recv, v_loc, t_send, t_recv, t_loc,
           rs_send, rs_recv, ag_send, ag_recv, g_sems, p_send, p_recv, o_sem, vfree):
    NL = xT.shape[1]
    M = NL // H
    TB = H // 64
    K = H // 2
    S = H // 8
    ZP = H // 128
    FLAT = M - 5
    me = lax.axis_index('row')
    e = lax.axis_index('col')
    px, py = lax.rem(me, 2), me // 2
    peers = [py * 2 + (1 - px), (1 - py) * 2 + px, 3 - me]
    mine = pl.ds(pl.multiple_of(me * SH, SH), SH)

    def rows_of(t):
        return pl.ds(pl.multiple_of(t * H, H), H)

    def chunk(c):
        return pl.ds(pl.multiple_of(c * C, C), C)

    def lo_v(q):
        return jnp.maximum(q - 1, 0) // TB

    def own(q):
        return lax.rem(q, 2) == e

    def z_remote(k, p):
        return pltpu.make_async_remote_copy(
            src_ref=z_hbm.at[:, pl.ds(pl.multiple_of(peers[p] * NL + k * 128, 128), 128)],
            dst_ref=xT.at[chunk(me), pl.ds(pl.multiple_of(k * 128, 128), 128)],
            send_sem=z_send.at[k, p], recv_sem=z_recv.at[k, p],
            device_id=(peers[p], e), device_id_type=MESH)

    def z_local(k):
        return pltpu.make_async_copy(
            z_hbm.at[:, pl.ds(pl.multiple_of(me * NL + k * 128, 128), 128)],
            xT.at[chunk(me), pl.ds(pl.multiple_of(k * 128, 128), 128)], z_loc.at[k])

    def v_remote(q, t):
        s = lax.rem(q, 2)
        return pltpu.make_async_remote_copy(
            src_ref=v_hbm.at[rows_of(t), pl.ds(pl.multiple_of(q * 128, 128), 128)],
            dst_ref=vst.at[s, e, rows_of(t), :],
            send_sem=v_send.at[s, t], recv_sem=v_recv.at[s, t],
            device_id=(me, 1 - e), device_id_type=MESH)

    def v_local(q, t):
        s = lax.rem(q, 2)
        return pltpu.make_async_copy(
            v_hbm.at[rows_of(t), pl.ds(pl.multiple_of(q * 128, 128), 128)],
            vst.at[s, e, rows_of(t), :], v_loc.at[s, t])

    def t_remote(q):
        s = lax.rem(q, 4)
        return pltpu.make_async_remote_copy(
            src_ref=t_hbm.at[q], dst_ref=tst.at[s, e], send_sem=t_send.at[s], recv_sem=t_recv.at[s],
            device_id=(me, 1 - e), device_id_type=MESH)

    def t_local(q):
        s = lax.rem(q, 4)
        return pltpu.make_async_copy(t_hbm.at[q], tst.at[s, e], t_loc.at[s])

    def t01_copy(q):
        s = lax.rem(q // 2, 2)
        return pltpu.make_async_remote_copy(
            src_ref=t01s.at[s], dst_ref=t01r.at[s], send_sem=p_send.at[s], recv_sem=p_recv.at[s],
            device_id=(me, 1 - e), device_id_type=MESH)

    def rs_copy(c, p):
        return pltpu.make_async_remote_copy(
            src_ref=wsend.at[c, pl.ds(pl.multiple_of(peers[p] * SH, SH), SH), :],
            dst_ref=wrecv.at[c, p], send_sem=rs_send.at[c, p], recv_sem=rs_recv.at[c, p],
            device_id=(peers[p], e), device_id_type=MESH)

    def ag_copy(c, p):
        return pltpu.make_async_remote_copy(
            src_ref=ysend.at[c], dst_ref=yT.at[c, mine, :],
            send_sem=ag_send.at[c, p], recv_sem=ag_recv.at[c, p],
            device_id=(peers[p], e), device_id_type=MESH)

    def grs_copy(p):
        return pltpu.make_async_remote_copy(
            src_ref=gsend.at[pl.ds(pl.multiple_of(peers[p] * SH, SH), SH), :],
            dst_ref=grecv.at[p], send_sem=g_sems.at[0, p], recv_sem=g_sems.at[1, p],
            device_id=(peers[p], e), device_id_type=MESH)

    def gag_copy(p):
        return pltpu.make_async_remote_copy(
            src_ref=gown, dst_ref=gfull.at[mine, :], send_sem=g_sems.at[2, p], recv_sem=g_sems.at[3, p],
            device_id=(peers[p], e), device_id_type=MESH)

    def over_tiles(q, fn):
        def one(t, _):
            fn(q, t)
            return 0
        lax.fori_loop(lo_v(q), M, one, 0)

    def fetch(q):
        def one(q, t):
            v_remote(q, t).start()
            v_local(q, t).start()
        over_tiles(q, one)
        t_remote(q).start()
        t_local(q).start()

    def arrived(q):
        def one(q, t):
            v_local(q, t).wait()
            v_remote(q, t).wait_recv()
        over_tiles(q, one)
        t_local(q).wait()
        t_remote(q).wait_recv()

    def sent(q):
        over_tiles(q, lambda q, t: v_remote(q, t).wait_send())
        t_remote(q).wait_send()

    def release(q):
        pl.semaphore_signal(vfree, inc=1, device_id=(me, 1 - e), device_id_type=MESH)
        sent(q)
        pl.semaphore_wait(vfree, 1)
        fetch(q - 2)

    def prep(q, r0, n):
        s, s4 = lax.rem(q, 2), lax.rem(q, 4)
        rows = pl.ds(pl.multiple_of(r0, 16), n)
        for h in range(2):
            for k, piece in enumerate(split3(vst[s, h, rows, :])):
                vb[s4, k, rows, h * 128:(h + 1) * 128] = piece

    def add_gram(q, r0, n):
        s = lax.rem(q, 2)
        rows = pl.ds(pl.multiple_of(r0, 16), n)
        v0t = jnp.concatenate(split3(vst[s, 0, rows, :].T), axis=0)
        gacc[...] += dot6(128, v0t, *split3(vst[s, 1, rows, :]))

    def g_start(q):
        gsend[...] = gacc[...]
        for p in range(3):
            grs_copy(p).start()

    def g_mid(q):
        for p in range(3):
            grs_copy(p).wait_recv()
        g = (gsend[mine, :] + grecv[0]) + (grecv[1] + grecv[2])
        gown[...] = g
        gfull[mine, :] = g
        for p in range(3):
            gag_copy(p).start()

    def g_fin(q):
        for p in range(3):
            gag_copy(p).wait_recv()
            grs_copy(p).wait_send()
            gag_copy(p).wait_send()
        s = lax.rem(q, 4)
        u = lax.dot_general(tst[s, 0], gfull[...], NN, precision=HIGHEST, preferred_element_type=F32)
        t01 = -lax.dot_general(u, tst[s, 1], NN, precision=HIGHEST, preferred_element_type=F32)
        t01s[lax.rem(q // 2, 2)] = t01
        t01_copy(q).start()

    def t_build(q):
        s, s2, sh = lax.rem(q, 4), lax.rem(q, 2), lax.rem(q // 2, 2)

        def put(t01):
            tt = jnp.concatenate([
                jnp.concatenate([tst[s, 0].T, jnp.zeros((128, 128), F32)], axis=1),
                jnp.concatenate([t01.T, tst[s, 1].T], axis=1)], axis=0)
            for k, piece in enumerate(split3(tt)):
                tp[s2, k] = piece

        @pl.when(own(q))
        def _():
            t01_copy(q).wait_send()
            put(t01s[sh])

        @pl.when(jnp.logical_not(own(q)))
        def _():
            t01_copy(q).wait_recv()
            put(t01r[sh])

    def upd(b, c, r0, j, n=K):
        s4 = lax.rem(b, 4)
        rows = pl.ds(pl.multiple_of(r0, n), n)
        x = xT[chunk(c), rows] - dot6(C, ysp[...], vb[s4, 0, rows, :], vb[s4, 1, rows, :], vb[s4, 2, rows, :], NT)
        xT[chunk(c), rows] = x
        if j is not None:
            for i, piece in enumerate(split3(x)):
                xs[j, i * C:(i + 1) * C, :] = piece

    def wprod(q, r0, j):
        s4 = lax.rem(q, 4)
        rows = pl.ds(pl.multiple_of(r0, K), K)
        return dot6(C, xs[j], vb[s4, 0, rows, :], vb[s4, 1, rows, :], vb[s4, 2, rows, :])

    def body(b, c, r0, v0, units, gram, first, pend):
        q3 = jnp.maximum(b - 3, 0)
        slots = [0, 1, 2, 3][4 - units:]
        tail = []
        for s in range(units):
            back = s - 2
            if back < 0 and pend is not None:
                tail.append(wprod(pend[0], NL + back * K, 4 + back))
                if len(tail) == 2:
                    wsend[pend[1]] = (wacc[0] + tail[0]) + (wacc[1] + tail[1])
            elif back < 0 and not first:
                wacc[s % 2] += wprod(b - 1, r0 + back * K, 4 + back)
            upd(b, c, r0 + s * K, slots[s])
            if back >= 0:
                d = wprod(b - 1, r0 + back * K, slots[back])
                if first:
                    wacc[s % 2] = d
                else:
                    wacc[s % 2] += d
            prep(q3, v0 + s * S, S)
        if gram:
            add_gram(q3, v0, units * S)
        if first and units == 2:
            wacc[...] = jnp.zeros_like(wacc)

    def rs_wait(j):
        for p in range(3):
            rs_copy(lax.rem(j, 4), p).wait_recv()

    def rs_sum(j):
        c = lax.rem(j, 4)
        s2 = lax.rem(NB - 1 - j // 4, 2)
        w = (wsend[c, mine, :] + wrecv[c, 0]) + (wrecv[c, 1] + wrecv[c, 2])
        y = dot6(SH, jnp.concatenate(split3(w), axis=0), tp[s2, 0], tp[s2, 1], tp[s2, 2])
        ysend[c] = y
        yT[c, mine, :] = y

    def y_send(j):
        for p in range(3):
            ag_copy(lax.rem(j, 4), p).start()

    def w_send(c):
        for p in range(3):
            rs_copy(c, p).start()

    def y_take(c):
        for p in range(3):
            ag_copy(c, p).wait_recv()
            ag_copy(c, p).wait_send()
            rs_copy(c, p).wait_send()
        for i, piece in enumerate(split3(yT[c])):
            ysp[i * C:(i + 1) * C, :] = piece

    def z_start(k):
        for p in range(3):
            z_remote(k, p).start()
        z_local(k).start()

    def z_wait(t):
        def one(k, _):
            z_local(k).wait()
            for p in range(3):
                z_remote(k, p).wait_recv()
            return 0
        lax.fori_loop(t * ZP, (t + 1) * ZP, one, 0)

    barrier = pltpu.get_barrier_semaphore()
    for p in range(3):
        pl.semaphore_signal(barrier, inc=1, device_id=(peers[p], e), device_id_type=MESH)
    pl.semaphore_signal(barrier, inc=1, device_id=(me, 1 - e), device_id_type=MESH)
    pl.semaphore_wait(barrier, 4)

    fetch(NB - 1)
    fetch(NB - 2)

    def z_first(n, _):
        z_start(M * ZP - 1 - n)
        return 0
    lax.fori_loop(0, ZP, z_first, 0)

    def prep_all(q):
        arrived(q)

        def one(t, _):
            add_gram(q, t * H, H)
            prep(q, t * H, H)
            return 0

        gacc[...] = jnp.zeros_like(gacc)
        lax.fori_loop(lo_v(q), M, one, 0)

    def when_own(q, fn):
        @pl.when(own(q))
        def _():
            fn(q)

    prep_all(NB - 1)
    when_own(NB - 1, g_start)
    release(NB - 1)
    prep_all(NB - 2)
    when_own(NB - 2, g_start)
    release(NB - 2)
    when_own(NB - 1, g_mid)
    when_own(NB - 2, g_mid)
    when_own(NB - 1, g_fin)
    when_own(NB - 2, g_fin)
    prep_all(NB - 3)
    when_own(NB - 3, g_start)
    t_build(NB - 1)
    release(NB - 3)
    z_wait(M - 1)

    def first_w(c, _):
        for n in range(2):
            for i, piece in enumerate(split3(xT[chunk(c), NL - (2 - n) * K:NL - (1 - n) * K])):
                xs[2 + n, i * C:(i + 1) * C, :] = piece
        wsend[c] = wprod(NB - 1, NL - 2 * K, 2) + wprod(NB - 1, NL - K, 3)
        w_send(c)
        return 0
    lax.fori_loop(0, 4, first_w, 0)
    for j in range(2):
        rs_wait(j)
        rs_sum(j)
        y_send(j)

    FIRST = TB * (FLAT + 1)

    def slot(i, _):
        b = NB - 1 - i // 4
        c = lax.rem(i, 4)
        lo = (b - 1) // TB
        q3 = b - 3

        @pl.when(c == 0)
        def _():
            @pl.when(lax.rem(b, TB) == 0)
            def _():
                z_wait(lo)

            back = TB * (lo + 1) - 1 - b

            @pl.when(jnp.logical_and(jnp.logical_and(lo >= 1, back >= 0), lax.rem(back, TB // ZP) == 0))
            def _():
                z_start(lo * ZP - 1 - back // (TB // ZP))

            @pl.when(q3 >= 0)
            def _():
                arrived(q3)
                gacc[...] = jnp.zeros_like(gacc)

        @pl.when(c == 1)
        def _():
            @pl.when(jnp.logical_and(own(b - 2), b >= 2))
            def _():
                g_mid(b - 2)
            t_build(b - 1)

        with_gram = jnp.logical_and(q3 >= 0, own(q3))
        m = M - lo
        odd = lax.rem(m, 2)
        flat = lo <= FLAT
        base = lo * H
        v0 = base + c * (m * 2 * S)

        def above(t, _):
            r0 = t * H + c * (2 * S)

            @pl.when(with_gram)
            def _():
                add_gram(q3, r0, 2 * S)
            prep(q3, r0, 2 * S)
            return 0
        lax.fori_loop(jnp.where(q3 >= 0, lo_v(q3), lo), lo, above, 0)

        y_take(c)

        def first_body(gram, pend):
            for units in (2, 4):
                @pl.when(odd == (units == 2))
                def _():
                    body(b, c, base, v0, units, gram, True, pend)

        def more(gram, start, stop):
            def tile(k, _):
                body(b, c, base + (2 - odd) * H + k * (2 * H), v0 + ((2 - odd) * 2 + 4 * k) * S, 4, gram, False, None)
                return 0
            lax.fori_loop(start, stop, tile, 0)

        whole = (m + odd) // 2 - 1

        for gram in (True, False):
            @pl.when(jnp.logical_and(jnp.logical_not(flat), with_gram == gram))
            def _():
                first_body(gram, None)
                more(gram, 0, whole)

        @pl.when(jnp.logical_not(flat))
        def _():
            rs_wait(i + 2)
            rs_sum(i + 2)
            wsend[c] = (wacc[0] + wprod(b - 1, NL - 2 * K, 2)) + (wacc[1] + wprod(b - 1, NL - K, 3))
            y_send(i + 2)
            w_send(c)

        before = lax.rem(c + 3, 4)
        begin = jnp.logical_and(b == FIRST, c == 0)
        pend = (jnp.where(c == 0, b, b - 1), jnp.where(begin, 4, before))

        for gram in (True, False):
            @pl.when(jnp.logical_and(flat, with_gram == gram))
            def _():
                first_body(gram, pend)

                @pl.when(jnp.logical_not(begin))
                def _():
                    w_send(before)
                more(gram, 0, 1)
                rs_wait(i + 2)
                rs_sum(i + 2)
                y_send(i + 2)
                more(gram, 1, whole)

        @pl.when(c == 3)
        def _():
            @pl.when(jnp.logical_and(own(b - 2), b >= 2))
            def _():
                g_fin(b - 2)

            @pl.when(with_gram)
            def _():
                g_start(q3)

            @pl.when(q3 >= 2)
            def _():
                release(q3)
        return 0

    lax.fori_loop(0, 4 * (NB - 1), slot, 0)
    wsend[3] = (wacc[0] + wprod(0, NL - 2 * K, 2)) + (wacc[1] + wprod(0, NL - K, 3))
    w_send(3)

    def out_copy(c):
        return pltpu.make_async_copy(xT.at[chunk(c), :], out_hbm.at[chunk(c), :], o_sem.at[c])

    def end_slot(c, _):
        @pl.when(c < 2)
        def _():
            j = 4 * (NB - 1) + c + 2
            rs_wait(j)
            rs_sum(j)
            y_send(j)
        y_take(c)

        def tile(t, _):
            upd(0, c, t * 2 * H, None, 2 * H)
            return 0
        lax.fori_loop(0, M // 2, tile, 0)
        out_copy(c).start()
        return 0
    lax.fori_loop(0, 4, end_slot, 0)

    for c in range(4):
        out_copy(c).wait()

    def z_sent(k, _):
        for p in range(3):
            z_remote(k, p).wait_send()
        return 0
    lax.fori_loop(0, M * ZP, z_sent, 0)
    sent(1)
    sent(0)


def solution(mesh):
    def local_apply(v_loc, t_loc, z_loc):
        NL, half = v_loc.shape
        NB = half // 128
        H = min(512, NL // 8)
        tiles = NL // H
        z_t = z_loc.T
        any_ = pl.BlockSpec(memory_space=pl.ANY)
        dma = pltpu.SemaphoreType.DMA
        vmem = pltpu.VMEM
        x_t = pl.pallas_call(
            functools.partial(kernel, H, NB),
            out_shape=jax.ShapeDtypeStruct((4 * C, NL), F32),
            in_specs=[any_] * 3,
            out_specs=any_,
            scratch_shapes=[
                vmem((4 * C, NL), F32),
                vmem((2, 2, NL, 128), F32),
                vmem((4, 3, NL, B), BF16),
                vmem((4, 2, 128, 128), F32),
                vmem((2, 3, B, B), BF16),
                vmem((3 * C, B), BF16),
                vmem((4, 3 * C, H // 2), BF16),
                vmem((2, C, B), F32),
                vmem((5, C, B), F32),
                vmem((4, 3, SH, B), F32),
                vmem((4, SH, B), F32),
                vmem((4, C, B), F32),
                vmem((128, 128), F32),
                vmem((128, 128), F32),
                vmem((3, SH, 128), F32),
                vmem((SH, 128), F32),
                vmem((128, 128), F32),
                vmem((2, 128, 128), F32),
                vmem((2, 128, 128), F32),
                dma((NL // 128, 3)), dma((NL // 128, 3)), dma((NL // 128,)),
                dma((2, tiles)), dma((2, tiles)), dma((2, tiles)),
                dma((4,)), dma((4,)), dma((4,)),
                dma((4, 3)), dma((4, 3)), dma((4, 3)), dma((4, 3)),
                dma((4, 3)), dma((2,)), dma((2,)), dma((4,)),
                pltpu.SemaphoreType.REGULAR,
            ],
            compiler_params=pltpu.CompilerParams(
                collective_id=0, has_side_effects=True, vmem_limit_bytes=62 * 1024 * 1024),
            name='back_transform',
        )(t_loc, v_loc, z_t)
        return x_t.T

    return jax.shard_map(local_apply, mesh=mesh,
                         in_specs=(P('row', 'col'), P('col', None, None), P(None, ('col', 'row'))),
                         out_specs=P('row', 'col'), check_vma=False)
```

```python
import functools

import jax
import jax.numpy as jnp
from jax import lax
from jax.experimental import pallas as pl
from jax.experimental.pallas import tpu as pltpu
from jax.sharding import PartitionSpec as P

F32 = jnp.float32
BF16 = jnp.bfloat16
MESH = pl.DeviceIdType.MESH
NN = (((1,), (0,)), ((), ()))
NT = (((1,), (1,)), ((), ()))
C = 128
B = 256
SH = 32
CORES, CHIPS3, CHIPS4 = range(2), range(3), range(4)
FLAT_FROM = 5
TAIL = 4


def loop(start, stop, fn):
    def step(i, carry):
        fn(i)
        return carry
    lax.fori_loop(start, stop, step, 0)


def dg(a, b, dims=NN):
    return lax.dot_general(a, b, dims, preferred_element_type=F32)


def split3(x):
    x0 = x.astype(BF16)
    r1 = x - x0.astype(F32)
    x1 = r1.astype(BF16)
    x2 = (r1 - x1.astype(F32)).astype(BF16)
    return x0, x1, x2


def dot6(m, stack, b0, b1, b2, dims=NN):
    p = dg(stack[0:3 * m], b0, dims)
    q = dg(stack[0:2 * m], b1, dims)
    r = dg(stack[0:m], b2, dims)
    return p[0:m] + (p[m:2 * m] + q[0:m]) + (p[2 * m:] + q[m:] + r)


def kernel(H, NB, t_hbm, v_hbm, z_hbm, out_hbm,
           xT, vst, vb, tst, tp, ysp, xs, wacc, wsend, wrecv, ysend, yT,
           gacc, gsend, grecv, gown, gfull, t01s, t01r, vtail, ttail, xtail,
           z_send, z_recv, z_loc, v_send, v_recv, v_loc, t_send, t_recv, t_loc,
           rs_send, rs_recv, ag_send, ag_recv, g_sems, p_send, p_recv, o_sem, e_sems, d_sems, l_sem, x_sems, vfree):
    NL = xT.shape[1]
    M = NL // H
    TB = H // 64
    K = H // 2
    S = H // 8
    ZP = H // 128
    B0 = NB - 1 - TAIL
    RT = 64 * TAIL
    ZE = (NL - RT) // 128
    FLAT = FLAT_FROM
    me = lax.axis_index('row')
    e = lax.axis_index('col')
    px, py = lax.rem(me, 2), me // 2
    peers = [py * 2 + (1 - px), (1 - py) * 2 + px, 3 - me]
    mine = pl.ds(pl.multiple_of(me * SH, SH), SH)

    def rows_of(t):
        return pl.ds(pl.multiple_of(t * H, H), H)

    def chunk(c):
        return pl.ds(pl.multiple_of(c * C, C), C)

    def lo_v(q):
        return jnp.maximum(q - 1, 0) // TB

    def own(q):
        return lax.rem(q, 2) == e

    def z_remote(k, p):
        return pltpu.make_async_remote_copy(
            src_ref=z_hbm.at[:, pl.ds(pl.multiple_of(peers[p] * NL + k * 128, 128), 128)],
            dst_ref=xT.at[chunk(me), pl.ds(pl.multiple_of(k * 128, 128), 128)],
            send_sem=z_send.at[k, p], recv_sem=z_recv.at[k, p],
            device_id=(peers[p], e), device_id_type=MESH)

    def z_local(k):
        return pltpu.make_async_copy(
            z_hbm.at[:, pl.ds(pl.multiple_of(me * NL + k * 128, 128), 128)],
            xT.at[chunk(me), pl.ds(pl.multiple_of(k * 128, 128), 128)], z_loc.at[k])

    def v_remote(q, t):
        s = lax.rem(q, 2)
        return pltpu.make_async_remote_copy(
            src_ref=v_hbm.at[rows_of(t), pl.ds(pl.multiple_of(q * 128, 128), 128)],
            dst_ref=vst.at[s, e, rows_of(t), :],
            send_sem=v_send.at[s, t], recv_sem=v_recv.at[s, t],
            device_id=(me, 1 - e), device_id_type=MESH)

    def v_local(q, t):
        s = lax.rem(q, 2)
        return pltpu.make_async_copy(
            v_hbm.at[rows_of(t), pl.ds(pl.multiple_of(q * 128, 128), 128)],
            vst.at[s, e, rows_of(t), :], v_loc.at[s, t])

    def t_remote(q):
        s = lax.rem(q, 4)
        return pltpu.make_async_remote_copy(
            src_ref=t_hbm.at[q], dst_ref=tst.at[s, e], send_sem=t_send.at[s], recv_sem=t_recv.at[s],
            device_id=(me, 1 - e), device_id_type=MESH)

    def t_local(q):
        s = lax.rem(q, 4)
        return pltpu.make_async_copy(t_hbm.at[q], tst.at[s, e], t_loc.at[s])

    def t01_copy(q):
        s = lax.rem(q // 2, 2)
        return pltpu.make_async_remote_copy(
            src_ref=t01s.at[s], dst_ref=t01r.at[s], send_sem=p_send.at[s], recv_sem=p_recv.at[s],
            device_id=(me, 1 - e), device_id_type=MESH)

    def rs_copy(c, p):
        return pltpu.make_async_remote_copy(
            src_ref=wsend.at[c, pl.ds(pl.multiple_of(peers[p] * SH, SH), SH), :],
            dst_ref=wrecv.at[c, p], send_sem=rs_send.at[c, p], recv_sem=rs_recv.at[c, p],
            device_id=(peers[p], e), device_id_type=MESH)

    def ag_copy(c, p):
        return pltpu.make_async_remote_copy(
            src_ref=ysend.at[c], dst_ref=yT.at[c, mine, :],
            send_sem=ag_send.at[c, p], recv_sem=ag_recv.at[c, p],
            device_id=(peers[p], e), device_id_type=MESH)

    def grs_copy(p):
        return pltpu.make_async_remote_copy(
            src_ref=gsend.at[pl.ds(pl.multiple_of(peers[p] * SH, SH), SH), :],
            dst_ref=grecv.at[p], send_sem=g_sems.at[0, p], recv_sem=g_sems.at[1, p],
            device_id=(peers[p], e), device_id_type=MESH)

    def gag_copy(p):
        return pltpu.make_async_remote_copy(
            src_ref=gown, dst_ref=gfull.at[mine, :], send_sem=g_sems.at[2, p], recv_sem=g_sems.at[3, p],
            device_id=(peers[p], e), device_id_type=MESH)

    def top(k):
        return 64 * k // 128 * 128

    def e_remote(k, p):
        n = RT - top(k)
        return pltpu.make_async_remote_copy(
            src_ref=v_hbm.at[NL - n:, (B0 + 1 + k) * 128:(B0 + 2 + k) * 128],
            dst_ref=vtail.at[k, e, me, RT - n:, :],
            send_sem=e_sems.at[0, k, p], recv_sem=e_sems.at[1, k, p],
            device_id=(peers[p], e), device_id_type=MESH)

    def e_local(k):
        n = RT - top(k)
        return pltpu.make_async_copy(
            v_hbm.at[NL - n:, (B0 + 1 + k) * 128:(B0 + 2 + k) * 128],
            vtail.at[k, e, me, RT - n:, :], l_sem.at[0, k])

    def d_remote(k, p):
        n = RT - top(k)
        if p == 3:
            src, chip = v_hbm.at[NL - n:, (B0 + 1 + k) * 128:(B0 + 2 + k) * 128], me
        else:
            chip = peers[p]
            src = vtail.at[k, e, chip, RT - n:, :]
        return pltpu.make_async_remote_copy(
            src_ref=src, dst_ref=vtail.at[k, e, chip, RT - n:, :],
            send_sem=d_sems.at[0, k, p], recv_sem=d_sems.at[1, k, p],
            device_id=(me, 1 - e), device_id_type=MESH)

    def f_remote(k):
        return pltpu.make_async_remote_copy(
            src_ref=t_hbm.at[B0 + 1 + k], dst_ref=ttail.at[k, e],
            send_sem=d_sems.at[0, k, 4], recv_sem=d_sems.at[1, k, 4],
            device_id=(me, 1 - e), device_id_type=MESH)

    def f_local(k):
        return pltpu.make_async_copy(t_hbm.at[B0 + 1 + k], ttail.at[k, e], l_sem.at[1, k])

    def h_local(d):
        return pltpu.make_async_copy(z_hbm.at[:, (d + 1) * NL - RT:(d + 1) * NL], xtail.at[:, d * RT:(d + 1) * RT],
                                     l_sem.at[2, d])

    def x_remote(p):
        return pltpu.make_async_remote_copy(
            src_ref=xtail.at[:, pl.ds(pl.multiple_of(peers[p] * RT, RT), RT)],
            dst_ref=xT.at[chunk(me), NL - RT:], send_sem=x_sems.at[0, p], recv_sem=x_sems.at[1, p],
            device_id=(peers[p], e), device_id_type=MESH)

    def over_tiles(q, fn):
        def one(t):
            fn(q, t)
        loop(lo_v(q), M, one)

    def fetch(q):
        def one(q, t):
            v_remote(q, t).start()
            v_local(q, t).start()
        over_tiles(q, one)
        t_remote(q).start()
        t_local(q).start()

    def arrived(q):
        def one(q, t):
            v_local(q, t).wait()
            v_remote(q, t).wait_recv()
        over_tiles(q, one)
        t_local(q).wait()
        t_remote(q).wait_recv()

    def sent(q):
        over_tiles(q, lambda q, t: v_remote(q, t).wait_send())
        t_remote(q).wait_send()

    def release(q):
        pl.semaphore_signal(vfree, inc=1, device_id=(me, 1 - e), device_id_type=MESH)
        sent(q)
        pl.semaphore_wait(vfree, 1)
        fetch(q - 2)

    def prep(q, r0, n):
        s, s4 = lax.rem(q, 2), lax.rem(q, 4)
        rows = pl.ds(pl.multiple_of(r0, 16), n)
        for h in CORES:
            for k, piece in enumerate(split3(vst[s, h, rows, :])):
                vb[s4, k, rows, h * 128:(h + 1) * 128] = piece

    def add_gram(q, r0, n):
        s = lax.rem(q, 2)
        rows = pl.ds(pl.multiple_of(r0, 16), n)
        v0t = jnp.concatenate(split3(vst[s, 0, rows, :].T), axis=0)
        gacc[...] += dot6(128, v0t, *split3(vst[s, 1, rows, :]))

    def g_start(q):
        gsend[...] = gacc[...]
        for p in CHIPS3:
            grs_copy(p).start()

    def g_mid(q):
        for p in CHIPS3:
            grs_copy(p).wait_recv()
        g = (gsend[mine, :] + grecv[0]) + (grecv[1] + grecv[2])
        gown[...] = g
        gfull[mine, :] = g
        for p in CHIPS3:
            gag_copy(p).start()

    def g_fin(q):
        for p in CHIPS3:
            gag_copy(p).wait_recv()
            grs_copy(p).wait_send()
            gag_copy(p).wait_send()
        s = lax.rem(q, 4)
        t01 = t_cross(tst[s, 0], gfull[...], tst[s, 1])
        t01s[lax.rem(q // 2, 2)] = t01
        t01_copy(q).start()

    def t_put(s2, t0, t1, t01):
        tt = jnp.concatenate([
            jnp.concatenate([t0.T, jnp.zeros((128, 128), F32)], axis=1),
            jnp.concatenate([t01.T, t1.T], axis=1)], axis=0)
        for k, piece in enumerate(split3(tt)):
            tp[s2, k] = piece

    def t_cross(t0, g, t1):
        u = dot6(128, jnp.concatenate(split3(t0), axis=0), *split3(g))
        return -dot6(128, jnp.concatenate(split3(u), axis=0), *split3(t1))

    def t_build(q):
        s, s2, sh = lax.rem(q, 4), lax.rem(q, 2), lax.rem(q // 2, 2)

        @pl.when(own(q))
        def _():
            t01_copy(q).wait_send()
            t_put(s2, tst[s, 0], tst[s, 1], t01s[sh])

        @pl.when(jnp.logical_not(own(q)))
        def _():
            t01_copy(q).wait_recv()
            t_put(s2, tst[s, 0], tst[s, 1], t01r[sh])

    def upd(b, c, r0, j, n=K):
        s4 = lax.rem(b, 4)
        rows = pl.ds(pl.multiple_of(r0, n), n)
        x = xT[chunk(c), rows] - dot6(C, ysp[...], vb[s4, 0, rows, :], vb[s4, 1, rows, :], vb[s4, 2, rows, :], NT)
        xT[chunk(c), rows] = x
        if j is not None:
            for i, piece in enumerate(split3(x)):
                xs[j, i * C:(i + 1) * C, :] = piece

    def wprod(q, r0, j):
        s4 = lax.rem(q, 4)
        rows = pl.ds(pl.multiple_of(r0, K), K)
        return dot6(C, xs[j], vb[s4, 0, rows, :], vb[s4, 1, rows, :], vb[s4, 2, rows, :])

    def body(b, c, r0, v0, units, gram, first):
        q3 = jnp.maximum(b - 3, 0)
        slots = [0, 1, 2, 3][4 - units:]
        for s in range(units):
            back = s - 2
            if back < 0 and not first:
                wacc[s % 2] += wprod(b - 1, r0 + back * K, 4 + back)
            upd(b, c, r0 + s * K, slots[s])
            if back >= 0:
                d = wprod(b - 1, r0 + back * K, slots[back])
                if first:
                    wacc[s % 2] = d
                else:
                    wacc[s % 2] += d
            prep(q3, v0 + s * S, S)
        if gram:
            add_gram(q3, v0, units * S)
        if first and units == 2:
            wacc[...] = jnp.zeros_like(wacc)

    def half(b, c, m, v0, second, pend, gram):
        q3 = jnp.maximum(b - 3, 0)
        base = NL - m * H
        cut = m // 2 * 2
        for s in range(cut, 2 * m) if second else range(cut):
            back = s - 2
            if back < 0:
                d = wprod(pend[0], NL + back * K, 4 + back)
                if back == -2:
                    held = d
                else:
                    wsend[pend[1]] = (wacc[0] + held) + (wacc[1] + d)
            upd(b, c, base + s * K, (s - 2 * m) % 4)
            if back >= 0:
                d = wprod(b - 1, base + back * K, (back - 2 * m) % 4)
                if back < 2:
                    wacc[back] = d
                else:
                    wacc[back % 2] += d
            prep(q3, v0 + s * S, S)
        if gram:
            for n in range(0, 2 * m, 4):
                add_gram(q3, v0 + n * S, min(4, 2 * m - n) * S)

    def rs_wait(j):
        for p in CHIPS3:
            rs_copy(lax.rem(j, 4), p).wait_recv()

    def rs_sum(j):
        c = lax.rem(j, 4)
        s2 = lax.rem(B0 - j // 4, 2)
        w = (wsend[c, mine, :] + wrecv[c, 0]) + (wrecv[c, 1] + wrecv[c, 2])
        y = dot6(SH, jnp.concatenate(split3(w), axis=0), tp[s2, 0], tp[s2, 1], tp[s2, 2])
        ysend[c] = y
        yT[c, mine, :] = y

    def y_send(j):
        for p in CHIPS3:
            ag_copy(lax.rem(j, 4), p).start()

    def w_send(c):
        for p in CHIPS3:
            rs_copy(c, p).start()

    def y_take(c):
        for p in CHIPS3:
            ag_copy(c, p).wait_recv()
            ag_copy(c, p).wait_send()
            rs_copy(c, p).wait_send()
        for i, piece in enumerate(split3(yT[c])):
            ysp[i * C:(i + 1) * C, :] = piece

    def z_start(k):
        for p in CHIPS3:
            z_remote(k, p).start()
        z_local(k).start()

    def z_wait(t):
        def one(k):
            z_local(k).wait()
            for p in CHIPS3:
                z_remote(k, p).wait_recv()
        loop(t * ZP, (t + 1) * ZP, one)

    barrier = pltpu.get_barrier_semaphore()
    for p in CHIPS3:
        pl.semaphore_signal(barrier, inc=1, device_id=(peers[p], e), device_id_type=MESH)
    pl.semaphore_signal(barrier, inc=1, device_id=(me, 1 - e), device_id_type=MESH)
    pl.semaphore_wait(barrier, 4)

    for k in reversed(range(TAIL)):
        for p in CHIPS3:
            e_remote(k, p).start()
        e_local(k).start()
        d_remote(k, 3).start()
        f_remote(k).start()
        f_local(k).start()
    for d in CHIPS4:
        h_local(d).start()
    fetch(B0)
    fetch(B0 - 1)

    def z_first(n):
        z_start(ZE - 1 - n)
    ZS = (B0 - 1) // TB * ZP
    late = TB - 1 - (B0 - 1) % TB - 1
    step = TB // ZP
    loop(0, ZE - ZS + (late + step - 1) // step, z_first)

    def prep_all(q):
        arrived(q)

        def one(t):
            add_gram(q, t * H, H)
            prep(q, t * H, H)

        gacc[...] = jnp.zeros_like(gacc)
        loop(lo_v(q), M, one)

    def when_own(q, fn):
        @pl.when(own(q))
        def _():
            fn(q)

    def corner_pass(k):
        for p in CHIPS3:
            e_remote(k, p).wait_recv()
            d_remote(k, p).start()

    def corner(k):
        o = top(k)
        n = RT - o
        free = (B0 + 1) % 4
        e_local(k).wait()
        f_local(k).wait()
        f_remote(k).wait_recv()
        for p in CHIPS4:
            d_remote(k, p).wait_recv()
        gacc[...] = jnp.zeros_like(gacc)

        def split_chip(d):
            rows = pl.ds(pl.multiple_of(d * n, 128), n)
            f0, f1 = vtail[k, 0, d, o:, :], vtail[k, 1, d, o:, :]
            p0, p1 = split3(f0), split3(f1)
            for j in CHIPS3:
                vb[free, j, rows, 0:128] = p0[j]
                vb[free, j, rows, 128:256] = p1[j]
            gacc[...] += dot6(128, jnp.concatenate(split3(f0.T), axis=0), *p1)
        loop(0, 4, split_chip)
        t_put(0, ttail[k, 0], ttail[k, 1], t_cross(ttail[k, 0], gacc[...], ttail[k, 1]))
        w = None
        for d in CHIPS4:
            x = jnp.concatenate(split3(xtail[:, d * RT + o:(d + 1) * RT]), axis=0)
            r = slice(d * n, (d + 1) * n)
            part = dot6(C, x, vb[free, 0, r, :], vb[free, 1, r, :], vb[free, 2, r, :])
            w = part if w is None else w + part
        y = dot6(C, jnp.concatenate(split3(w), axis=0), tp[0, 0], tp[0, 1], tp[0, 2])
        for i, piece in enumerate(split3(y)):
            ysp[i * C:(i + 1) * C, :] = piece
        for d in CHIPS4:
            r = slice(d * n, (d + 1) * n)
            xtail[:, d * RT + o:(d + 1) * RT] -= dot6(
                C, ysp[...], vb[free, 0, r, :], vb[free, 1, r, :], vb[free, 2, r, :], NT)

    prep_all(B0)
    when_own(B0, g_start)
    release(B0)
    prep_all(B0 - 1)
    when_own(B0 - 1, g_start)
    release(B0 - 1)
    for d in CHIPS4:
        h_local(d).wait()
    corner_pass(TAIL - 1)
    for k in reversed(range(TAIL)):
        if k:
            corner_pass(k - 1)
        corner(k)
    for p in CHIPS3:
        x_remote(p).start()
    xT[chunk(me), NL - RT:] = xtail[:, pl.ds(pl.multiple_of(me * RT, RT), RT)]
    when_own(B0, g_mid)
    when_own(B0 - 1, g_mid)
    when_own(B0, g_fin)
    when_own(B0 - 1, g_fin)
    prep_all(B0 - 2)
    when_own(B0 - 2, g_start)
    t_build(B0)
    release(B0 - 2)

    def z_first_wait(k):
        z_local(k).wait()
        for p in CHIPS3:
            z_remote(k, p).wait_recv()
    loop(ZS, ZE, z_first_wait)
    for p in CHIPS3:
        x_remote(p).wait_recv()

    def first_w(c):
        wacc[...] = jnp.zeros_like(wacc)

        def one(t):
            for n in CORES:
                r0 = t * H + n * K
                for i, piece in enumerate(split3(xT[chunk(c), pl.ds(pl.multiple_of(r0, K), K)])):
                    xs[2 + n, i * C:(i + 1) * C, :] = piece
                wacc[n] += wprod(B0, r0, 2 + n)
        loop(B0 // TB, M, one)
        wsend[c] = wacc[0] + wacc[1]
        w_send(c)
    loop(0, 4, first_w)
    for j in CORES:
        rs_wait(j)
        rs_sum(j)
        y_send(j)

    FIRST = TB * (M - FLAT + 1)

    def slot(i):
        b = B0 - i // 4
        c = lax.rem(i, 4)
        lo = (b - 1) // TB
        q3 = b - 3

        @pl.when(c == 0)
        def _():
            @pl.when(lax.rem(b, TB) == 0)
            def _():
                z_wait(lo)

            back = TB * (lo + 1) - 1 - b

            @pl.when(jnp.logical_and(jnp.logical_and(lo >= 1, back >= 0), lax.rem(back, TB // ZP) == 0))
            def _():
                z_start(lo * ZP - 1 - back // (TB // ZP))

            @pl.when(q3 >= 0)
            def _():
                arrived(q3)
                gacc[...] = jnp.zeros_like(gacc)

        @pl.when(c == 1)
        def _():
            @pl.when(jnp.logical_and(own(b - 2), b >= 2))
            def _():
                g_mid(b - 2)
            t_build(b - 1)

        with_gram = jnp.logical_and(q3 >= 0, own(q3))
        m = M - lo
        base = lo * H
        v0 = base + c * (m * 2 * S)

        def above(t):
            r0 = t * H + c * (2 * S)

            @pl.when(with_gram)
            def _():
                add_gram(q3, r0, 2 * S)
            prep(q3, r0, 2 * S)
        loop(jnp.where(q3 >= 0, lo_v(q3), lo), lo, above)

        before = lax.rem(c + 3, 4)
        begin = jnp.logical_and(b == FIRST, c == 0)
        pend = (jnp.where(c == 0, b, b - 1), jnp.where(begin, 4, before))

        def start(m, gram):
            @pl.when(with_gram == gram)
            def _():
                y_take(c)
                if m >= FLAT:
                    half(b, c, m, v0, False, pend, gram)
                else:
                    body(b, c, base, v0, 4 - m % 2 * 2, gram, True)

        for odd in (0, 1):
            @pl.when(jnp.logical_and(lo > M - FLAT, lax.rem(m, 2) == odd))
            def _():
                for gram in (True, False):
                    start(odd, gram)

                    @pl.when(with_gram == gram)
                    def _():
                        def tile(k):
                            n = 2 - odd + 2 * k
                            body(b, c, base + n * H, v0 + 2 * n * S, 4, gram, False)
                        loop(0, (m + odd) // 2 - 1, tile)
                rs_wait(i + 2)
                rs_sum(i + 2)
                wsend[c] = (wacc[0] + wprod(b - 1, NL - 2 * K, 2)) + (wacc[1] + wprod(b - 1, NL - K, 3))
                y_send(i + 2)
                w_send(c)

        for tiles in range(FLAT, M + 1):
            @pl.when(m == tiles)
            def _():
                for gram in (True, False):
                    start(tiles, gram)

                @pl.when(jnp.logical_not(begin))
                def _():
                    w_send(before)
                rs_wait(i + 2)
                rs_sum(i + 2)
                half(b, c, tiles, v0, True, None, False)
                y_send(i + 2)

        @pl.when(c == 3)
        def _():
            @pl.when(jnp.logical_and(own(b - 2), b >= 2))
            def _():
                g_fin(b - 2)

            @pl.when(with_gram)
            def _():
                g_start(q3)

            @pl.when(q3 >= 2)
            def _():
                release(q3)

    loop(0, 4 * B0, slot)
    if FLAT <= M:
        wsend[3] = (wacc[0] + wprod(0, NL - 2 * K, 2)) + (wacc[1] + wprod(0, NL - K, 3))
        w_send(3)

    def out_copy(c):
        return pltpu.make_async_copy(xT.at[chunk(c), :], out_hbm.at[chunk(c), :], o_sem.at[c])

    def end_slot(c):
        @pl.when(c < 2)
        def _():
            j = 4 * B0 + c + 2
            rs_wait(j)
            rs_sum(j)
            y_send(j)
        y_take(c)

        def tile(t):
            upd(0, c, t * 2 * H, None, 2 * H)
        loop(0, M // 2, tile)
        out_copy(c).start()
    loop(0, 4, end_slot)

    for c in range(4):
        out_copy(c).wait()

    def z_sent(k):
        for p in CHIPS3:
            z_remote(k, p).wait_send()
    loop(0, ZE, z_sent)
    for p in CHIPS3:
        x_remote(p).wait_send()
        for k in range(TAIL):
            e_remote(k, p).wait_send()
    for k in range(TAIL):
        f_remote(k).wait_send()
        for p in CHIPS4:
            d_remote(k, p).wait_send()
    sent(1)
    sent(0)


def solution(mesh):
    def local_apply(v_loc, t_loc, z_loc):
        NL, half = v_loc.shape
        NB = half // 128
        H = min(512, NL // 8)
        tiles = NL // H
        z_t = z_loc.T
        any_ = pl.BlockSpec(memory_space=pl.ANY)
        dma = pltpu.SemaphoreType.DMA
        vmem = pltpu.VMEM
        x_t = pl.pallas_call(
            functools.partial(kernel, H, NB),
            out_shape=jax.ShapeDtypeStruct((4 * C, NL), F32),
            in_specs=[any_] * 3,
            out_specs=any_,
            scratch_shapes=[
                vmem((4 * C, NL), F32),
                vmem((2, 2, NL, 128), F32),
                vmem((4, 3, NL, B), BF16),
                vmem((4, 2, 128, 128), F32),
                vmem((2, 3, B, B), BF16),
                vmem((3 * C, B), BF16),
                vmem((4, 3 * C, H // 2), BF16),
                vmem((2, C, B), F32),
                vmem((5, C, B), F32),
                vmem((4, 3, SH, B), F32),
                vmem((4, SH, B), F32),
                vmem((4, C, B), F32),
                vmem((128, 128), F32),
                vmem((128, 128), F32),
                vmem((3, SH, 128), F32),
                vmem((SH, 128), F32),
                vmem((128, 128), F32),
                vmem((2, 128, 128), F32),
                vmem((2, 128, 128), F32),
                vmem((TAIL, 2, 4, 64 * TAIL, 128), F32),
                vmem((TAIL, 2, 128, 128), F32),
                vmem((C, 4 * 64 * TAIL), F32),
                dma((NL // 128, 3)), dma((NL // 128, 3)), dma((NL // 128,)),
                *[dma((2, tiles))] * 3, *[dma((4,))] * 3,
                *[dma((4, 3))] * 5, dma((2,)), dma((2,)), dma((4,)),
                dma((2, TAIL, 3)), dma((2, TAIL, 5)), dma((3, max(TAIL, 4))), dma((2, 3)),
                pltpu.SemaphoreType.REGULAR,
            ],
            compiler_params=pltpu.CompilerParams(
                collective_id=0, has_side_effects=True, vmem_limit_bytes=62 * 1024 * 1024),
            name='back_transform',
        )(t_loc, v_loc, z_t)
        return x_t.T

    return jax.shard_map(local_apply, mesh=mesh,
                         in_specs=(P('row', 'col'), P('col', None, None), P(None, ('col', 'row'))),
                         out_specs=P('row', 'col'), check_vma=False)
```

```python
import functools

import jax
import jax.numpy as jnp
from jax import lax
from jax.experimental import pallas as pl
from jax.experimental.pallas import tpu as pltpu
from jax.sharding import PartitionSpec as P

F32 = jnp.float32
BF16 = jnp.bfloat16
MESH = pl.DeviceIdType.MESH
NN = (((1,), (0,)), ((), ()))
NT = (((1,), (1,)), ((), ()))
C = 128
B = 256
SH = 32
CORES, CHIPS3, CHIPS4 = range(2), range(3), range(4)
FLAT_FROM = 5
TAIL = 6


def loop(start, stop, fn):
    def step(i, carry):
        fn(i)
        return carry
    lax.fori_loop(start, stop, step, 0)


def dg(a, b, dims=NN):
    return lax.dot_general(a, b, dims, preferred_element_type=F32)


def split3(x):
    x0 = x.astype(BF16)
    r1 = x - x0.astype(F32)
    x1 = r1.astype(BF16)
    x2 = (r1 - x1.astype(F32)).astype(BF16)
    return x0, x1, x2


def dot6(m, stack, b0, b1, b2, dims=NN):
    p = dg(stack[0:3 * m], b0, dims)
    q = dg(stack[0:2 * m], b1, dims)
    r = dg(stack[0:m], b2, dims)
    return p[0:m] + (p[m:2 * m] + q[0:m]) + (p[2 * m:] + q[m:] + r)


def kernel(H, NB, t_hbm, v_hbm, z_hbm, out_hbm,
           xT, vst, vb, tst, tp, ysp, xs, wacc, wsend, wrecv, ysend, yT,
           gacc, gsend, grecv, gown, gfull, t01s, t01r, vtail, ttail, xtail,
           z_send, z_recv, z_loc, v_send, v_recv, v_loc, t_send, t_recv, t_loc,
           rs_send, rs_recv, ag_send, ag_recv, g_sems, p_send, p_recv, o_sem, e_sems, d_sems, l_sem, x_sems, vfree):
    NL = xT.shape[1]
    M = NL // H
    TB = H // 64
    K = H // 2
    S = H // 8
    ZP = H // 128
    B0 = NB - 1 - TAIL
    RT = 64 * TAIL
    ZE = (NL - RT) // 128
    FLAT = FLAT_FROM
    me = lax.axis_index('row')
    e = lax.axis_index('col')
    px, py = lax.rem(me, 2), me // 2
    peers = [py * 2 + (1 - px), (1 - py) * 2 + px, 3 - me]
    mine = pl.ds(pl.multiple_of(me * SH, SH), SH)

    def rows_of(t):
        return pl.ds(pl.multiple_of(t * H, H), H)

    def chunk(c):
        return pl.ds(pl.multiple_of(c * C, C), C)

    def lo_v(q):
        return jnp.maximum(q - 1, 0) // TB

    def own(q):
        return lax.rem(q, 2) == e

    def z_remote(k, p):
        return pltpu.make_async_remote_copy(
            src_ref=z_hbm.at[:, pl.ds(pl.multiple_of(peers[p] * NL + k * 128, 128), 128)],
            dst_ref=xT.at[chunk(me), pl.ds(pl.multiple_of(k * 128, 128), 128)],
            send_sem=z_send.at[k, p], recv_sem=z_recv.at[k, p],
            device_id=(peers[p], e), device_id_type=MESH)

    def z_local(k):
        return pltpu.make_async_copy(
            z_hbm.at[:, pl.ds(pl.multiple_of(me * NL + k * 128, 128), 128)],
            xT.at[chunk(me), pl.ds(pl.multiple_of(k * 128, 128), 128)], z_loc.at[k])

    def v_remote(q, t):
        s = lax.rem(q, 2)
        return pltpu.make_async_remote_copy(
            src_ref=v_hbm.at[rows_of(t), pl.ds(pl.multiple_of(q * 128, 128), 128)],
            dst_ref=vst.at[s, e, rows_of(t), :],
            send_sem=v_send.at[s, t], recv_sem=v_recv.at[s, t],
            device_id=(me, 1 - e), device_id_type=MESH)

    def v_local(q, t):
        s = lax.rem(q, 2)
        return pltpu.make_async_copy(
            v_hbm.at[rows_of(t), pl.ds(pl.multiple_of(q * 128, 128), 128)],
            vst.at[s, e, rows_of(t), :], v_loc.at[s, t])

    def t_remote(q):
        s = lax.rem(q, 4)
        return pltpu.make_async_remote_copy(
            src_ref=t_hbm.at[q], dst_ref=tst.at[s, e], send_sem=t_send.at[s], recv_sem=t_recv.at[s],
            device_id=(me, 1 - e), device_id_type=MESH)

    def t_local(q):
        s = lax.rem(q, 4)
        return pltpu.make_async_copy(t_hbm.at[q], tst.at[s, e], t_loc.at[s])

    def t01_copy(q):
        s = lax.rem(q // 2, 2)
        return pltpu.make_async_remote_copy(
            src_ref=t01s.at[s], dst_ref=t01r.at[s], send_sem=p_send.at[s], recv_sem=p_recv.at[s],
            device_id=(me, 1 - e), device_id_type=MESH)

    def rs_copy(c, p):
        return pltpu.make_async_remote_copy(
            src_ref=wsend.at[c, pl.ds(pl.multiple_of(peers[p] * SH, SH), SH), :],
            dst_ref=wrecv.at[c, p], send_sem=rs_send.at[c, p], recv_sem=rs_recv.at[c, p],
            device_id=(peers[p], e), device_id_type=MESH)

    def ag_copy(c, p):
        return pltpu.make_async_remote_copy(
            src_ref=ysend.at[c], dst_ref=yT.at[c, mine, :],
            send_sem=ag_send.at[c, p], recv_sem=ag_recv.at[c, p],
            device_id=(peers[p], e), device_id_type=MESH)

    def grs_copy(p):
        return pltpu.make_async_remote_copy(
            src_ref=gsend.at[pl.ds(pl.multiple_of(peers[p] * SH, SH), SH), :],
            dst_ref=grecv.at[p], send_sem=g_sems.at[0, p], recv_sem=g_sems.at[1, p],
            device_id=(peers[p], e), device_id_type=MESH)

    def gag_copy(p):
        return pltpu.make_async_remote_copy(
            src_ref=gown, dst_ref=gfull.at[mine, :], send_sem=g_sems.at[2, p], recv_sem=g_sems.at[3, p],
            device_id=(peers[p], e), device_id_type=MESH)

    def e_ref(k, g):
        return v_hbm.at[NL - RT + g * 128:, pl.ds(pl.multiple_of((B0 + 1 + k) * 128, 128), 128)]

    def e_remote(k, g, p):
        return pltpu.make_async_remote_copy(
            src_ref=e_ref(k, g), dst_ref=vtail.at[k, e, me, g * 128:, :],
            send_sem=e_sems.at[0, k, p], recv_sem=e_sems.at[1, k, p],
            device_id=(peers[p], e), device_id_type=MESH)

    def e_local(k, g):
        return pltpu.make_async_copy(e_ref(k, g), vtail.at[k, e, me, g * 128:, :], l_sem.at[0, k])

    def d_remote(k, g, p):
        chip = me if p == 3 else peers[p]
        src = e_ref(k, g) if p == 3 else vtail.at[k, e, chip, g * 128:, :]
        return pltpu.make_async_remote_copy(
            src_ref=src, dst_ref=vtail.at[k, e, chip, g * 128:, :],
            send_sem=d_sems.at[0, k, p], recv_sem=d_sems.at[1, k, p],
            device_id=(me, 1 - e), device_id_type=MESH)

    def f_remote(k):
        return pltpu.make_async_remote_copy(
            src_ref=t_hbm.at[B0 + 1 + k], dst_ref=ttail.at[k, e],
            send_sem=d_sems.at[0, k, 4], recv_sem=d_sems.at[1, k, 4],
            device_id=(me, 1 - e), device_id_type=MESH)

    def f_local(k):
        return pltpu.make_async_copy(t_hbm.at[B0 + 1 + k], ttail.at[k, e], l_sem.at[1, k])

    def h_local(d):
        return pltpu.make_async_copy(z_hbm.at[:, (d + 1) * NL - RT:(d + 1) * NL], xtail.at[:, d * RT:(d + 1) * RT],
                                     l_sem.at[2, d])

    def x_remote(p):
        return pltpu.make_async_remote_copy(
            src_ref=xtail.at[:, pl.ds(pl.multiple_of(peers[p] * RT, RT), RT)],
            dst_ref=xT.at[chunk(me), NL - RT:], send_sem=x_sems.at[0, p], recv_sem=x_sems.at[1, p],
            device_id=(peers[p], e), device_id_type=MESH)

    def over_tiles(q, fn):
        def one(t):
            fn(q, t)
        loop(lo_v(q), M, one)

    def fetch(q):
        def one(q, t):
            v_remote(q, t).start()
            v_local(q, t).start()
        over_tiles(q, one)
        t_remote(q).start()
        t_local(q).start()

    def arrived(q):
        def one(q, t):
            v_local(q, t).wait()
            v_remote(q, t).wait_recv()
        over_tiles(q, one)
        t_local(q).wait()
        t_remote(q).wait_recv()

    def sent(q):
        over_tiles(q, lambda q, t: v_remote(q, t).wait_send())
        t_remote(q).wait_send()

    def release(q):
        pl.semaphore_signal(vfree, inc=1, device_id=(me, 1 - e), device_id_type=MESH)

    def refill(q):
        sent(q)
        pl.semaphore_wait(vfree, 1)
        fetch(q - 2)

    def prep(q, r0, n):
        s, s4 = lax.rem(q, 2), lax.rem(q, 4)
        rows = pl.ds(pl.multiple_of(r0, 16), n)
        for h in CORES:
            for k, piece in enumerate(split3(vst[s, h, rows, :])):
                vb[s4, k, rows, h * 128:(h + 1) * 128] = piece

    def add_gram(q, r0, n):
        s = lax.rem(q, 2)
        rows = pl.ds(pl.multiple_of(r0, 16), n)
        v0t = jnp.concatenate(split3(vst[s, 0, rows, :].T), axis=0)
        gacc[...] += dot6(128, v0t, *split3(vst[s, 1, rows, :]))

    def g_start(q):
        gsend[...] = gacc[...]
        for p in CHIPS3:
            grs_copy(p).start()

    def g_mid(q):
        for p in CHIPS3:
            grs_copy(p).wait_recv()
        g = (gsend[mine, :] + grecv[0]) + (grecv[1] + grecv[2])
        gown[...] = g
        gfull[mine, :] = g
        for p in CHIPS3:
            gag_copy(p).start()

    def g_fin(q):
        for p in CHIPS3:
            gag_copy(p).wait_recv()
            grs_copy(p).wait_send()
            gag_copy(p).wait_send()
        s = lax.rem(q, 4)
        t01 = t_cross(tst[s, 0], gfull[...], tst[s, 1])
        t01s[lax.rem(q // 2, 2)] = t01
        t01_copy(q).start()

    def t_put(s2, t0, t1, t01):
        tt = jnp.concatenate([
            jnp.concatenate([t0.T, jnp.zeros((128, 128), F32)], axis=1),
            jnp.concatenate([t01.T, t1.T], axis=1)], axis=0)
        for k, piece in enumerate(split3(tt)):
            tp[s2, k] = piece

    def t_cross(t0, g, t1):
        u = dot6(128, jnp.concatenate(split3(t0), axis=0), *split3(g))
        return -dot6(128, jnp.concatenate(split3(u), axis=0), *split3(t1))

    def t_build(q):
        s, s2, sh = lax.rem(q, 4), lax.rem(q, 2), lax.rem(q // 2, 2)

        @pl.when(own(q))
        def _():
            t01_copy(q).wait_send()
            t_put(s2, tst[s, 0], tst[s, 1], t01s[sh])

        @pl.when(jnp.logical_not(own(q)))
        def _():
            t01_copy(q).wait_recv()
            t_put(s2, tst[s, 0], tst[s, 1], t01r[sh])

    def upd(b, c, r0, j, n=K):
        s4 = lax.rem(b, 4)
        rows = pl.ds(pl.multiple_of(r0, n), n)
        x = xT[chunk(c), rows] - dot6(C, ysp[...], vb[s4, 0, rows, :], vb[s4, 1, rows, :], vb[s4, 2, rows, :], NT)
        xT[chunk(c), rows] = x
        if j is not None:
            for i, piece in enumerate(split3(x)):
                xs[j, i * C:(i + 1) * C, :] = piece

    def wprod(q, r0, j):
        s4 = lax.rem(q, 4)
        rows = pl.ds(pl.multiple_of(r0, K), K)
        return dot6(C, xs[j], vb[s4, 0, rows, :], vb[s4, 1, rows, :], vb[s4, 2, rows, :])

    def body(b, c, r0, v0, units, gram, first):
        q3 = jnp.maximum(b - 3, 0)
        slots = [0, 1, 2, 3][4 - units:]
        for s in range(units):
            back = s - 2
            if back < 0 and not first:
                wacc[s % 2] += wprod(b - 1, r0 + back * K, 4 + back)
            upd(b, c, r0 + s * K, slots[s])
            if back >= 0:
                d = wprod(b - 1, r0 + back * K, slots[back])
                if first:
                    wacc[s % 2] = d
                else:
                    wacc[s % 2] += d
            prep(q3, v0 + s * S, S)
        if gram:
            add_gram(q3, v0, units * S)
        if first and units == 2:
            wacc[...] = jnp.zeros_like(wacc)

    def half(b, c, m, v0, second, pend, gram):
        q3 = jnp.maximum(b - 3, 0)
        base = NL - m * H
        cut = m // 2 * 2
        for s in range(cut, 2 * m) if second else range(cut):
            back = s - 2
            if back < 0:
                d = wprod(pend[0], NL + back * K, 4 + back)
                if back == -2:
                    held = d
                else:
                    wsend[pend[1]] = (wacc[0] + held) + (wacc[1] + d)
            upd(b, c, base + s * K, (s - 2 * m) % 4)
            if back >= 0:
                d = wprod(b - 1, base + back * K, (back - 2 * m) % 4)
                if back < 2:
                    wacc[back] = d
                else:
                    wacc[back % 2] += d
            prep(q3, v0 + s * S, S)
        if gram:
            for n in range(0, 2 * m, 4):
                add_gram(q3, v0 + n * S, min(4, 2 * m - n) * S)

    def rs_wait(j):
        for p in CHIPS3:
            rs_copy(lax.rem(j, 4), p).wait_recv()

    def rs_sum(j):
        c = lax.rem(j, 4)
        s2 = lax.rem(B0 - j // 4, 2)
        w = (wsend[c, mine, :] + wrecv[c, 0]) + (wrecv[c, 1] + wrecv[c, 2])
        y = dot6(SH, jnp.concatenate(split3(w), axis=0), tp[s2, 0], tp[s2, 1], tp[s2, 2])
        ysend[c] = y
        yT[c, mine, :] = y

    def y_send(j):
        for p in CHIPS3:
            ag_copy(lax.rem(j, 4), p).start()

    def w_send(c):
        for p in CHIPS3:
            rs_copy(c, p).start()

    def y_take(c):
        for p in CHIPS3:
            ag_copy(c, p).wait_recv()
            ag_copy(c, p).wait_send()
            rs_copy(c, p).wait_send()
        for i, piece in enumerate(split3(yT[c])):
            ysp[i * C:(i + 1) * C, :] = piece

    def z_start(k):
        for p in CHIPS3:
            z_remote(k, p).start()
        z_local(k).start()

    def z_wait(t):
        def one(k):
            z_local(k).wait()
            for p in CHIPS3:
                z_remote(k, p).wait_recv()
        loop(t * ZP, (t + 1) * ZP, one)

    barrier = pltpu.get_barrier_semaphore()
    for p in CHIPS3:
        pl.semaphore_signal(barrier, inc=1, device_id=(peers[p], e), device_id_type=MESH)
    pl.semaphore_signal(barrier, inc=1, device_id=(me, 1 - e), device_id_type=MESH)
    pl.semaphore_wait(barrier, 4)

    for k in reversed(range(TAIL)):
        g = k // 2
        for p in CHIPS3:
            e_remote(k, g, p).start()
        e_local(k, g).start()
        d_remote(k, g, 3).start()
        f_remote(k).start()
        f_local(k).start()
    for d in CHIPS4:
        h_local(d).start()
    fetch(B0)
    fetch(B0 - 1)

    def z_first(n):
        z_start(ZE - 1 - n)
    ZS = (B0 - 1) // TB * ZP
    late = TB - 1 - (B0 - 1) % TB - 1
    step = TB // ZP
    loop(0, ZE - ZS + (late + step - 1) // step, z_first)

    def prep_all(q):
        arrived(q)

        def one(t):
            add_gram(q, t * H, H)
            prep(q, t * H, H)

        gacc[...] = jnp.zeros_like(gacc)
        loop(lo_v(q), M, one)

    def when_own(q, fn):
        @pl.when(own(q))
        def _():
            fn(q)

    def corner_pass(k, g):
        for p in CHIPS3:
            e_remote(k, g, p).wait_recv()
            d_remote(k, g, p).start()

    def corner(k, g):
        o = g * 128
        n = RT - o
        free = (B0 + 1) % 4
        e_local(k, g).wait()
        f_local(k).wait()
        f_remote(k).wait_recv()
        for p in CHIPS4:
            d_remote(k, g, p).wait_recv()
        gacc[...] = jnp.zeros_like(gacc)

        def split_chip(d):
            rows = pl.ds(pl.multiple_of(d * n, 128), n)
            f0, f1 = vtail[k, 0, d, o:, :], vtail[k, 1, d, o:, :]
            p0, p1 = split3(f0), split3(f1)
            for j in CHIPS3:
                vb[free, j, rows, 0:128] = p0[j]
                vb[free, j, rows, 128:256] = p1[j]
            gacc[...] += dot6(128, jnp.concatenate(split3(f0.T), axis=0), *p1)
        loop(0, 4, split_chip)
        t_put(0, ttail[k, 0], ttail[k, 1], t_cross(ttail[k, 0], gacc[...], ttail[k, 1]))
        w = None
        for d in CHIPS4:
            x = jnp.concatenate(split3(xtail[:, d * RT + o:(d + 1) * RT]), axis=0)
            r = slice(d * n, (d + 1) * n)
            part = dot6(C, x, vb[free, 0, r, :], vb[free, 1, r, :], vb[free, 2, r, :])
            w = part if w is None else w + part
        y = dot6(C, jnp.concatenate(split3(w), axis=0), tp[0, 0], tp[0, 1], tp[0, 2])
        for i, piece in enumerate(split3(y)):
            ysp[i * C:(i + 1) * C, :] = piece
        for d in CHIPS4:
            r = slice(d * n, (d + 1) * n)
            xtail[:, d * RT + o:(d + 1) * RT] -= dot6(
                C, ysp[...], vb[free, 0, r, :], vb[free, 1, r, :], vb[free, 2, r, :], NT)

    prep_all(B0)
    when_own(B0, g_start)
    release(B0)
    refill(B0)
    prep_all(B0 - 1)
    when_own(B0 - 1, g_start)
    release(B0 - 1)
    refill(B0 - 1)
    for d in CHIPS4:
        h_local(d).wait()
    for g in reversed(range(TAIL // 2)):
        corner_pass(2 * g + 1, g)

        def pair(n):
            @pl.when(n == 0)
            def _():
                corner_pass(2 * g, g)
            corner(2 * g + 1 - n, g)
        loop(0, 2, pair)
    for p in CHIPS3:
        x_remote(p).start()
    xT[chunk(me), NL - RT:] = xtail[:, pl.ds(pl.multiple_of(me * RT, RT), RT)]
    when_own(B0, g_mid)
    when_own(B0 - 1, g_mid)
    when_own(B0, g_fin)
    when_own(B0 - 1, g_fin)
    prep_all(B0 - 2)
    when_own(B0 - 2, g_start)
    t_build(B0)
    release(B0 - 2)

    def z_first_wait(k):
        z_local(k).wait()
        for p in CHIPS3:
            z_remote(k, p).wait_recv()
    loop(ZS, ZE, z_first_wait)
    for p in CHIPS3:
        x_remote(p).wait_recv()

    def first_w(c):
        wacc[...] = jnp.zeros_like(wacc)

        def one(t):
            for n in CORES:
                r0 = t * H + n * K
                for i, piece in enumerate(split3(xT[chunk(c), pl.ds(pl.multiple_of(r0, K), K)])):
                    xs[2 + n, i * C:(i + 1) * C, :] = piece
                wacc[n] += wprod(B0, r0, 2 + n)
        loop(B0 // TB, M, one)
        wsend[c] = wacc[0] + wacc[1]
        w_send(c)
    loop(0, 4, first_w)
    for j in CORES:
        rs_wait(j)
        rs_sum(j)
        y_send(j)

    FIRST = TB * (M - FLAT + 1)

    def slot(i):
        b = B0 - i // 4
        c = lax.rem(i, 4)
        lo = (b - 1) // TB
        q3 = b - 3

        @pl.when(c == 0)
        def _():
            @pl.when(lax.rem(b, TB) == 0)
            def _():
                z_wait(lo)

            back = TB * (lo + 1) - 1 - b

            @pl.when(jnp.logical_and(jnp.logical_and(lo >= 1, back >= 0), lax.rem(back, TB // ZP) == 0))
            def _():
                z_start(lo * ZP - 1 - back // (TB // ZP))

            @pl.when(q3 >= 0)
            def _():
                arrived(q3)
                gacc[...] = jnp.zeros_like(gacc)

        @pl.when(c == 1)
        def _():
            @pl.when(jnp.logical_and(own(b - 2), b >= 2))
            def _():
                g_mid(b - 2)
            t_build(b - 1)

            @pl.when(b >= 4)
            def _():
                refill(b - 2)

        with_gram = jnp.logical_and(q3 >= 0, own(q3))
        m = M - lo
        base = lo * H
        v0 = base + c * (m * 2 * S)

        def above(t):
            r0 = t * H + c * (2 * S)

            @pl.when(with_gram)
            def _():
                add_gram(q3, r0, 2 * S)
            prep(q3, r0, 2 * S)
        loop(jnp.where(q3 >= 0, lo_v(q3), lo), lo, above)

        before = lax.rem(c + 3, 4)
        begin = jnp.logical_and(b == FIRST, c == 0)
        pend = (jnp.where(c == 0, b, b - 1), jnp.where(begin, 4, before))

        def start(m, gram):
            @pl.when(with_gram == gram)
            def _():
                y_take(c)
                if m >= FLAT:
                    half(b, c, m, v0, False, pend, gram)
                else:
                    body(b, c, base, v0, 4 - m % 2 * 2, gram, True)

        for odd in (0, 1):
            @pl.when(jnp.logical_and(lo > M - FLAT, lax.rem(m, 2) == odd))
            def _():
                for gram in (True, False):
                    start(odd, gram)

                    @pl.when(with_gram == gram)
                    def _():
                        def tile(k):
                            n = 2 - odd + 2 * k
                            body(b, c, base + n * H, v0 + 2 * n * S, 4, gram, False)
                        loop(0, (m + odd) // 2 - 1, tile)
                rs_wait(i + 2)
                rs_sum(i + 2)
                wsend[c] = (wacc[0] + wprod(b - 1, NL - 2 * K, 2)) + (wacc[1] + wprod(b - 1, NL - K, 3))
                y_send(i + 2)
                w_send(c)

        for tiles in range(FLAT, M + 1):
            @pl.when(m == tiles)
            def _():
                for gram in (True, False):
                    start(tiles, gram)

                @pl.when(jnp.logical_not(begin))
                def _():
                    w_send(before)
                rs_wait(i + 2)
                rs_sum(i + 2)
                half(b, c, tiles, v0, True, None, False)
                y_send(i + 2)

        @pl.when(c == 3)
        def _():
            @pl.when(jnp.logical_and(own(b - 2), b >= 2))
            def _():
                g_fin(b - 2)

            @pl.when(with_gram)
            def _():
                g_start(q3)

            @pl.when(q3 >= 2)
            def _():
                release(q3)

    loop(0, 4 * B0, slot)
    if FLAT <= M:
        wsend[3] = (wacc[0] + wprod(0, NL - 2 * K, 2)) + (wacc[1] + wprod(0, NL - K, 3))
        w_send(3)

    def out_copy(c):
        return pltpu.make_async_copy(xT.at[chunk(c), :], out_hbm.at[chunk(c), :], o_sem.at[c])

    def end_slot(c):
        @pl.when(c < 2)
        def _():
            j = 4 * B0 + c + 2
            rs_wait(j)
            rs_sum(j)
            y_send(j)
        y_take(c)

        def tile(t):
            upd(0, c, t * 2 * H, None, 2 * H)
        loop(0, M // 2, tile)
        out_copy(c).start()
    loop(0, 4, end_slot)

    for c in range(4):
        out_copy(c).wait()

    def z_sent(k):
        for p in CHIPS3:
            z_remote(k, p).wait_send()
    loop(0, ZE, z_sent)
    for p in CHIPS3:
        x_remote(p).wait_send()
        for k in range(TAIL):
            e_remote(k, k // 2, p).wait_send()
    for k in range(TAIL):
        f_remote(k).wait_send()
        for p in CHIPS4:
            d_remote(k, k // 2, p).wait_send()
    sent(1)
    sent(0)


def solution(mesh):
    def local_apply(v_loc, t_loc, z_loc):
        NL, half = v_loc.shape
        NB = half // 128
        H = min(512, NL // 8)
        tiles = NL // H
        z_t = z_loc.T
        any_ = pl.BlockSpec(memory_space=pl.ANY)
        dma = pltpu.SemaphoreType.DMA
        vmem = pltpu.VMEM
        x_t = pl.pallas_call(
            functools.partial(kernel, H, NB),
            out_shape=jax.ShapeDtypeStruct((4 * C, NL), F32),
            in_specs=[any_] * 3,
            out_specs=any_,
            scratch_shapes=[
                vmem((4 * C, NL), F32),
                vmem((2, 2, NL, 128), F32),
                vmem((4, 3, NL, B), BF16),
                vmem((4, 2, 128, 128), F32),
                vmem((2, 3, B, B), BF16),
                vmem((3 * C, B), BF16),
                vmem((4, 3 * C, H // 2), BF16),
                vmem((2, C, B), F32),
                vmem((5, C, B), F32),
                vmem((4, 3, SH, B), F32),
                vmem((4, SH, B), F32),
                vmem((4, C, B), F32),
                vmem((128, 128), F32),
                vmem((128, 128), F32),
                vmem((3, SH, 128), F32),
                vmem((SH, 128), F32),
                vmem((128, 128), F32),
                vmem((2, 128, 128), F32),
                vmem((2, 128, 128), F32),
                vmem((TAIL, 2, 4, 64 * TAIL, 128), F32),
                vmem((TAIL, 2, 128, 128), F32),
                vmem((C, 4 * 64 * TAIL), F32),
                dma((NL // 128, 3)), dma((NL // 128, 3)), dma((NL // 128,)),
                *[dma((2, tiles))] * 3, *[dma((4,))] * 3,
                *[dma((4, 3))] * 5, dma((2,)), dma((2,)), dma((4,)),
                dma((2, TAIL, 3)), dma((2, TAIL, 5)), dma((3, max(TAIL, 4))), dma((2, 3)),
                pltpu.SemaphoreType.REGULAR,
            ],
            compiler_params=pltpu.CompilerParams(
                collective_id=0, has_side_effects=True, vmem_limit_bytes=62 * 1024 * 1024),
            name='back_transform',
        )(t_loc, v_loc, z_t)
        return x_t.T

    return jax.shard_map(local_apply, mesh=mesh,
                         in_specs=(P('row', 'col'), P('col', None, None), P(None, ('col', 'row'))),
                         out_specs=P('row', 'col'), check_vma=False)
```

```python
import functools

import jax
import jax.numpy as jnp
from jax import lax
from jax.experimental import pallas as pl
from jax.experimental.pallas import tpu as pltpu
from jax.sharding import PartitionSpec as P

F32 = jnp.float32
BF16 = jnp.bfloat16
MESH = pl.DeviceIdType.MESH
NN = (((1,), (0,)), ((), ()))
NT = (((1,), (1,)), ((), ()))
C = 128
B = 256
SH = 32
CORES, CHIPS3, CHIPS4 = range(2), range(3), range(4)
FLAT_FROM = 5
TAIL = 6


def loop(start, stop, fn):
    def step(i, carry):
        fn(i)
        return carry
    lax.fori_loop(start, stop, step, 0)


def dg(a, b, dims=NN):
    return lax.dot_general(a, b, dims, preferred_element_type=F32)


def split3(x):
    x0 = x.astype(BF16)
    r1 = x - x0.astype(F32)
    x1 = r1.astype(BF16)
    x2 = (r1 - x1.astype(F32)).astype(BF16)
    return x0, x1, x2


def dot6(m, stack, b0, b1, b2, dims=NN):
    p = dg(stack[0:3 * m], b0, dims)
    q = dg(stack[0:2 * m], b1, dims)
    r = dg(stack[0:m], b2, dims)
    return p[0:m] + (p[m:2 * m] + q[0:m]) + (p[2 * m:] + q[m:] + r)


def kernel(H, NB, t_hbm, v_hbm, z_hbm, out_hbm,
           xT, vst, vb, tst, tp, ysp, xs, wacc, wsend, wrecv, ysend, yT,
           gacc, gsend, grecv, gown, gfull, t01s, t01r, vtail, ttail, xtail, zst,
           z_send, z_recv, z_loc, z_in, v_send, v_recv, v_loc, t_send, t_recv, t_loc,
           rs_send, rs_recv, ag_send, ag_recv, g_sems, p_send, p_recv, o_sem, e_sems, d_sems, l_sem, x_sems, vfree):
    NL = xT.shape[1]
    M = NL // H
    TB = H // 64
    K = H // 2
    S = H // 8
    ZP = H // 128
    B0 = NB - 1 - TAIL
    RT = 64 * TAIL
    ZE = (NL - RT) // 128
    FLAT = FLAT_FROM
    me = lax.axis_index('row')
    e = lax.axis_index('col')
    px, py = lax.rem(me, 2), me // 2
    peers = [py * 2 + (1 - px), (1 - py) * 2 + px, 3 - me]
    mine = pl.ds(pl.multiple_of(me * SH, SH), SH)

    def rows_of(t):
        return pl.ds(pl.multiple_of(t * H, H), H)

    def chunk(c):
        return pl.ds(pl.multiple_of(c * C, C), C)

    def lo_v(q):
        return jnp.maximum(q - 1, 0) // TB

    def own(q):
        return lax.rem(q, 2) == e

    def z_load(k, p):
        return pltpu.make_async_copy(
            z_hbm.at[:, pl.ds(pl.multiple_of(peers[p] * NL + k * 128, 128), 128)],
            zst.at[lax.rem(k, 4), p], z_in.at[lax.rem(k, 4), p])

    def z_remote(k, p):
        return pltpu.make_async_remote_copy(
            src_ref=zst.at[lax.rem(k, 4), p],
            dst_ref=xT.at[chunk(me), pl.ds(pl.multiple_of(k * 128, 128), 128)],
            send_sem=z_send.at[k, p], recv_sem=z_recv.at[k, p],
            device_id=(peers[p], e), device_id_type=MESH)

    def z_local(k):
        return pltpu.make_async_copy(
            z_hbm.at[:, pl.ds(pl.multiple_of(me * NL + k * 128, 128), 128)],
            xT.at[chunk(me), pl.ds(pl.multiple_of(k * 128, 128), 128)], z_loc.at[k])

    def v_remote(q, t):
        s = lax.rem(q, 2)
        return pltpu.make_async_remote_copy(
            src_ref=v_hbm.at[rows_of(t), pl.ds(pl.multiple_of(q * 128, 128), 128)],
            dst_ref=vst.at[s, e, rows_of(t), :],
            send_sem=v_send.at[s, t], recv_sem=v_recv.at[s, t],
            device_id=(me, 1 - e), device_id_type=MESH)

    def v_local(q, t):
        s = lax.rem(q, 2)
        return pltpu.make_async_copy(
            v_hbm.at[rows_of(t), pl.ds(pl.multiple_of(q * 128, 128), 128)],
            vst.at[s, e, rows_of(t), :], v_loc.at[s, t])

    def t_remote(q):
        s = lax.rem(q, 4)
        return pltpu.make_async_remote_copy(
            src_ref=t_hbm.at[q], dst_ref=tst.at[s, e], send_sem=t_send.at[s], recv_sem=t_recv.at[s],
            device_id=(me, 1 - e), device_id_type=MESH)

    def t_local(q):
        s = lax.rem(q, 4)
        return pltpu.make_async_copy(t_hbm.at[q], tst.at[s, e], t_loc.at[s])

    def t01_copy(q):
        s = lax.rem(q // 2, 2)
        return pltpu.make_async_remote_copy(
            src_ref=t01s.at[s], dst_ref=t01r.at[s], send_sem=p_send.at[s], recv_sem=p_recv.at[s],
            device_id=(me, 1 - e), device_id_type=MESH)

    def rs_copy(c, p):
        return pltpu.make_async_remote_copy(
            src_ref=wsend.at[c, pl.ds(pl.multiple_of(peers[p] * SH, SH), SH), :],
            dst_ref=wrecv.at[c, p], send_sem=rs_send.at[c, p], recv_sem=rs_recv.at[c, p],
            device_id=(peers[p], e), device_id_type=MESH)

    def ag_copy(c, p):
        return pltpu.make_async_remote_copy(
            src_ref=ysend.at[c], dst_ref=yT.at[c, mine, :],
            send_sem=ag_send.at[c, p], recv_sem=ag_recv.at[c, p],
            device_id=(peers[p], e), device_id_type=MESH)

    def grs_copy(p):
        return pltpu.make_async_remote_copy(
            src_ref=gsend.at[pl.ds(pl.multiple_of(peers[p] * SH, SH), SH), :],
            dst_ref=grecv.at[p], send_sem=g_sems.at[0, p], recv_sem=g_sems.at[1, p],
            device_id=(peers[p], e), device_id_type=MESH)

    def gag_copy(p):
        return pltpu.make_async_remote_copy(
            src_ref=gown, dst_ref=gfull.at[mine, :], send_sem=g_sems.at[2, p], recv_sem=g_sems.at[3, p],
            device_id=(peers[p], e), device_id_type=MESH)

    def e_ref(k, g):
        return v_hbm.at[NL - RT + g * 128:, pl.ds(pl.multiple_of((B0 + 1 + k) * 128, 128), 128)]

    def e_remote(k, g, p):
        return pltpu.make_async_remote_copy(
            src_ref=vtail.at[k, e, me, g * 128:, :], dst_ref=vtail.at[k, e, me, g * 128:, :],
            send_sem=e_sems.at[0, k, p], recv_sem=e_sems.at[1, k, p],
            device_id=(peers[p], e), device_id_type=MESH)

    def e_local(k, g):
        return pltpu.make_async_copy(e_ref(k, g), vtail.at[k, e, me, g * 128:, :], l_sem.at[0, k])

    def d_remote(k, g, p):
        chip = me if p == 3 else peers[p]
        return pltpu.make_async_remote_copy(
            src_ref=vtail.at[k, e, chip, g * 128:, :], dst_ref=vtail.at[k, e, chip, g * 128:, :],
            send_sem=d_sems.at[0, k, p], recv_sem=d_sems.at[1, k, p],
            device_id=(me, 1 - e), device_id_type=MESH)

    def f_remote(k):
        return pltpu.make_async_remote_copy(
            src_ref=t_hbm.at[B0 + 1 + k], dst_ref=ttail.at[k, e],
            send_sem=d_sems.at[0, k, 4], recv_sem=d_sems.at[1, k, 4],
            device_id=(me, 1 - e), device_id_type=MESH)

    def f_local(k):
        return pltpu.make_async_copy(t_hbm.at[B0 + 1 + k], ttail.at[k, e], l_sem.at[1, k])

    def h_local(d):
        return pltpu.make_async_copy(z_hbm.at[:, (d + 1) * NL - RT:(d + 1) * NL], xtail.at[:, d * RT:(d + 1) * RT],
                                     l_sem.at[2, d])

    def x_remote(p):
        return pltpu.make_async_remote_copy(
            src_ref=xtail.at[:, pl.ds(pl.multiple_of(peers[p] * RT, RT), RT)],
            dst_ref=xT.at[chunk(me), NL - RT:], send_sem=x_sems.at[0, p], recv_sem=x_sems.at[1, p],
            device_id=(peers[p], e), device_id_type=MESH)

    def over_tiles(q, fn):
        def one(t):
            fn(q, t)
        loop(lo_v(q), M, one)

    def fetch(q):
        def one(q, t):
            v_remote(q, t).start()
            v_local(q, t).start()
        over_tiles(q, one)
        t_remote(q).start()
        t_local(q).start()

    def arrived(q):
        def one(q, t):
            v_local(q, t).wait()
            v_remote(q, t).wait_recv()
        over_tiles(q, one)
        t_local(q).wait()
        t_remote(q).wait_recv()

    def sent(q):
        over_tiles(q, lambda q, t: v_remote(q, t).wait_send())
        t_remote(q).wait_send()

    def release(q):
        pl.semaphore_signal(vfree, inc=1, device_id=(me, 1 - e), device_id_type=MESH)

    def refill(q):
        sent(q)
        pl.semaphore_wait(vfree, 1)
        fetch(q - 2)

    def prep(q, r0, n):
        s, s4 = lax.rem(q, 2), lax.rem(q, 4)
        rows = pl.ds(pl.multiple_of(r0, 16), n)
        for h in CORES:
            for k, piece in enumerate(split3(vst[s, h, rows, :])):
                vb[s4, k, rows, h * 128:(h + 1) * 128] = piece

    def add_gram(q, r0, n):
        s = lax.rem(q, 2)
        rows = pl.ds(pl.multiple_of(r0, 16), n)
        v0t = jnp.concatenate(split3(vst[s, 0, rows, :].T), axis=0)
        gacc[...] += dot6(128, v0t, *split3(vst[s, 1, rows, :]))

    def g_start(q):
        gsend[...] = gacc[...]
        for p in CHIPS3:
            grs_copy(p).start()

    def g_mid(q):
        for p in CHIPS3:
            grs_copy(p).wait_recv()
        g = (gsend[mine, :] + grecv[0]) + (grecv[1] + grecv[2])
        gown[...] = g
        gfull[mine, :] = g
        for p in CHIPS3:
            gag_copy(p).start()

    def g_fin(q):
        for p in CHIPS3:
            gag_copy(p).wait_recv()
            grs_copy(p).wait_send()
            gag_copy(p).wait_send()
        s = lax.rem(q, 4)
        t01 = t_cross(tst[s, 0], gfull[...], tst[s, 1])
        t01s[lax.rem(q // 2, 2)] = t01
        t01_copy(q).start()

    def t_put(s2, t0, t1, t01):
        tt = jnp.concatenate([
            jnp.concatenate([t0.T, jnp.zeros((128, 128), F32)], axis=1),
            jnp.concatenate([t01.T, t1.T], axis=1)], axis=0)
        for k, piece in enumerate(split3(tt)):
            tp[s2, k] = piece

    def t_cross(t0, g, t1):
        u = dot6(128, jnp.concatenate(split3(t0), axis=0), *split3(g))
        return -dot6(128, jnp.concatenate(split3(u), axis=0), *split3(t1))

    def t_build(q):
        s, s2, sh = lax.rem(q, 4), lax.rem(q, 2), lax.rem(q // 2, 2)

        @pl.when(own(q))
        def _():
            t01_copy(q).wait_send()
            t_put(s2, tst[s, 0], tst[s, 1], t01s[sh])

        @pl.when(jnp.logical_not(own(q)))
        def _():
            t01_copy(q).wait_recv()
            t_put(s2, tst[s, 0], tst[s, 1], t01r[sh])

    def upd(b, c, r0, j, n=K):
        s4 = lax.rem(b, 4)
        rows = pl.ds(pl.multiple_of(r0, n), n)
        x = xT[chunk(c), rows] - dot6(C, ysp[...], vb[s4, 0, rows, :], vb[s4, 1, rows, :], vb[s4, 2, rows, :], NT)
        xT[chunk(c), rows] = x
        if j is not None:
            for i, piece in enumerate(split3(x)):
                xs[j, i * C:(i + 1) * C, :] = piece

    def wprod(q, r0, j):
        s4 = lax.rem(q, 4)
        rows = pl.ds(pl.multiple_of(r0, K), K)
        return dot6(C, xs[j], vb[s4, 0, rows, :], vb[s4, 1, rows, :], vb[s4, 2, rows, :])

    def body(b, c, r0, v0, units, gram, first):
        q3 = jnp.maximum(b - 3, 0)
        slots = [0, 1, 2, 3][4 - units:]
        for s in range(units):
            back = s - 2
            if back < 0 and not first:
                wacc[s % 2] += wprod(b - 1, r0 + back * K, 4 + back)
            upd(b, c, r0 + s * K, slots[s])
            if back >= 0:
                d = wprod(b - 1, r0 + back * K, slots[back])
                if first:
                    wacc[s % 2] = d
                else:
                    wacc[s % 2] += d
            prep(q3, v0 + s * S, S)
        if gram:
            add_gram(q3, v0, units * S)
        if first and units == 2:
            wacc[...] = jnp.zeros_like(wacc)

    def half(b, c, m, v0, second, pend, gram):
        q3 = jnp.maximum(b - 3, 0)
        base = NL - m * H
        cut = m // 2 * 2
        for s in range(cut, 2 * m) if second else range(cut):
            back = s - 2
            if back < 0:
                d = wprod(pend[0], NL + back * K, 4 + back)
                if back == -2:
                    held = d
                else:
                    wsend[pend[1]] = (wacc[0] + held) + (wacc[1] + d)
            upd(b, c, base + s * K, (s - 2 * m) % 4)
            if back >= 0:
                d = wprod(b - 1, base + back * K, (back - 2 * m) % 4)
                if back < 2:
                    wacc[back] = d
                else:
                    wacc[back % 2] += d
            prep(q3, v0 + s * S, S)
        if gram:
            for n in range(0, 2 * m, 4):
                add_gram(q3, v0 + n * S, min(4, 2 * m - n) * S)

    def rs_wait(j):
        for p in CHIPS3:
            rs_copy(lax.rem(j, 4), p).wait_recv()

    def rs_sum(j):
        c = lax.rem(j, 4)
        s2 = lax.rem(B0 - j // 4, 2)
        w = (wsend[c, mine, :] + wrecv[c, 0]) + (wrecv[c, 1] + wrecv[c, 2])
        y = dot6(SH, jnp.concatenate(split3(w), axis=0), tp[s2, 0], tp[s2, 1], tp[s2, 2])
        ysend[c] = y
        yT[c, mine, :] = y

    def y_send(j):
        for p in CHIPS3:
            ag_copy(lax.rem(j, 4), p).start()

    def w_send(c):
        for p in CHIPS3:
            rs_copy(c, p).start()

    def y_take(c):
        for p in CHIPS3:
            ag_copy(c, p).wait_recv()
            ag_copy(c, p).wait_send()
            rs_copy(c, p).wait_send()
        for i, piece in enumerate(split3(yT[c])):
            ysp[i * C:(i + 1) * C, :] = piece

    def z_stage(k):
        @pl.when(k + 4 < ZE)
        def _():
            for p in CHIPS3:
                z_remote(k + 4, p).wait_send()
        for p in CHIPS3:
            z_load(k, p).start()
        z_local(k).start()

    def z_go(k):
        for p in CHIPS3:
            z_load(k, p).wait()
        for p in CHIPS3:
            z_remote(k, p).start()

    def z_wait(t):
        def one(k):
            z_local(k).wait()
            for p in CHIPS3:
                z_remote(k, p).wait_recv()
        loop(t * ZP, (t + 1) * ZP, one)

    barrier = pltpu.get_barrier_semaphore()
    for p in CHIPS3:
        pl.semaphore_signal(barrier, inc=1, device_id=(peers[p], e), device_id_type=MESH)
    pl.semaphore_signal(barrier, inc=1, device_id=(me, 1 - e), device_id_type=MESH)
    pl.semaphore_wait(barrier, 4)

    for k in reversed(range(TAIL)):
        e_local(k, k // 2).start()
        f_remote(k).start()
        f_local(k).start()
    for k in reversed(range(TAIL)):
        e_local(k, k // 2).wait()
        for p in CHIPS3:
            e_remote(k, k // 2, p).start()
        d_remote(k, k // 2, 3).start()
    for d in CHIPS4:
        h_local(d).start()
    fetch(B0)
    fetch(B0 - 1)

    def z_first(n):
        z_stage(ZE - 1 - n)

    def z_second(n):
        z_go(ZE - 1 - n)
    ZS = (B0 - 1) // TB * ZP
    late = TB - 1 - (B0 - 1) % TB - 1
    step = TB // ZP
    early = ZE - ZS + (late + step - 1) // step
    loop(0, early, z_first)
    loop(0, early, z_second)

    def prep_all(q):
        arrived(q)

        def one(t):
            add_gram(q, t * H, H)
            prep(q, t * H, H)

        gacc[...] = jnp.zeros_like(gacc)
        loop(lo_v(q), M, one)

    def when_own(q, fn):
        @pl.when(own(q))
        def _():
            fn(q)

    def corner_pass(k, g):
        for p in CHIPS3:
            e_remote(k, g, p).wait_recv()
            d_remote(k, g, p).start()

    def corner(k, g):
        o = g * 128
        n = RT - o
        free = (B0 + 1) % 4
        f_local(k).wait()
        f_remote(k).wait_recv()
        for p in CHIPS4:
            d_remote(k, g, p).wait_recv()
        gacc[...] = jnp.zeros_like(gacc)

        def split_chip(d):
            rows = pl.ds(pl.multiple_of(d * n, 128), n)
            f0, f1 = vtail[k, 0, d, o:, :], vtail[k, 1, d, o:, :]
            p0, p1 = split3(f0), split3(f1)
            for j in CHIPS3:
                vb[free, j, rows, 0:128] = p0[j]
                vb[free, j, rows, 128:256] = p1[j]
            gacc[...] += dot6(128, jnp.concatenate(split3(f0.T), axis=0), *p1)
        loop(0, 4, split_chip)
        t_put(0, ttail[k, 0], ttail[k, 1], t_cross(ttail[k, 0], gacc[...], ttail[k, 1]))
        w = None
        for d in CHIPS4:
            x = jnp.concatenate(split3(xtail[:, d * RT + o:(d + 1) * RT]), axis=0)
            r = slice(d * n, (d + 1) * n)
            part = dot6(C, x, vb[free, 0, r, :], vb[free, 1, r, :], vb[free, 2, r, :])
            w = part if w is None else w + part
        y = dot6(C, jnp.concatenate(split3(w), axis=0), tp[0, 0], tp[0, 1], tp[0, 2])
        for i, piece in enumerate(split3(y)):
            ysp[i * C:(i + 1) * C, :] = piece
        for d in CHIPS4:
            r = slice(d * n, (d + 1) * n)
            xtail[:, d * RT + o:(d + 1) * RT] -= dot6(
                C, ysp[...], vb[free, 0, r, :], vb[free, 1, r, :], vb[free, 2, r, :], NT)

    prep_all(B0)
    when_own(B0, g_start)
    release(B0)
    refill(B0)
    prep_all(B0 - 1)
    when_own(B0 - 1, g_start)
    release(B0 - 1)
    refill(B0 - 1)
    for d in CHIPS4:
        h_local(d).wait()
    for g in reversed(range(TAIL // 2)):
        corner_pass(2 * g + 1, g)

        def pair(n):
            @pl.when(n == 0)
            def _():
                corner_pass(2 * g, g)
            corner(2 * g + 1 - n, g)
        loop(0, 2, pair)
    for p in CHIPS3:
        x_remote(p).start()
    xT[chunk(me), NL - RT:] = xtail[:, pl.ds(pl.multiple_of(me * RT, RT), RT)]
    when_own(B0, g_mid)
    when_own(B0 - 1, g_mid)
    when_own(B0, g_fin)
    when_own(B0 - 1, g_fin)
    prep_all(B0 - 2)
    when_own(B0 - 2, g_start)
    t_build(B0)
    release(B0 - 2)

    def z_first_wait(k):
        z_local(k).wait()
        for p in CHIPS3:
            z_remote(k, p).wait_recv()
    loop(ZS, ZE, z_first_wait)
    for p in CHIPS3:
        x_remote(p).wait_recv()

    def first_w(c):
        wacc[...] = jnp.zeros_like(wacc)

        def one(t):
            for n in CORES:
                r0 = t * H + n * K
                for i, piece in enumerate(split3(xT[chunk(c), pl.ds(pl.multiple_of(r0, K), K)])):
                    xs[2 + n, i * C:(i + 1) * C, :] = piece
                wacc[n] += wprod(B0, r0, 2 + n)
        loop(B0 // TB, M, one)
        wsend[c] = wacc[0] + wacc[1]
        w_send(c)
    loop(0, 4, first_w)
    for j in CORES:
        rs_wait(j)
        rs_sum(j)
        y_send(j)

    FIRST = TB * (M - FLAT + 1)

    def slot(i):
        b = B0 - i // 4
        c = lax.rem(i, 4)
        lo = (b - 1) // TB
        q3 = b - 3

        back = TB * (lo + 1) - 1 - b
        z_now = jnp.logical_and(jnp.logical_and(lo >= 1, back >= 0), lax.rem(back, TB // ZP) == 0)
        z_piece = lo * ZP - 1 - back // (TB // ZP)

        @pl.when(c == 0)
        def _():
            @pl.when(lax.rem(b, TB) == 0)
            def _():
                z_wait(lo)

            @pl.when(z_now)
            def _():
                z_stage(z_piece)

            @pl.when(q3 >= 0)
            def _():
                arrived(q3)
                gacc[...] = jnp.zeros_like(gacc)

        @pl.when(c == 1)
        def _():
            @pl.when(z_now)
            def _():
                z_go(z_piece)

            @pl.when(jnp.logical_and(own(b - 2), b >= 2))
            def _():
                g_mid(b - 2)
            t_build(b - 1)

            @pl.when(b >= 4)
            def _():
                refill(b - 2)

        with_gram = jnp.logical_and(q3 >= 0, own(q3))
        m = M - lo
        base = lo * H
        v0 = base + c * (m * 2 * S)

        def above(t):
            r0 = t * H + c * (2 * S)

            @pl.when(with_gram)
            def _():
                add_gram(q3, r0, 2 * S)
            prep(q3, r0, 2 * S)
        loop(jnp.where(q3 >= 0, lo_v(q3), lo), lo, above)

        before = lax.rem(c + 3, 4)
        begin = jnp.logical_and(b == FIRST, c == 0)
        pend = (jnp.where(c == 0, b, b - 1), jnp.where(begin, 4, before))

        def start(m, gram):
            @pl.when(with_gram == gram)
            def _():
                y_take(c)
                if m >= FLAT:
                    half(b, c, m, v0, False, pend, gram)
                else:
                    body(b, c, base, v0, 4 - m % 2 * 2, gram, True)

        for odd in (0, 1):
            @pl.when(jnp.logical_and(lo > M - FLAT, lax.rem(m, 2) == odd))
            def _():
                for gram in (True, False):
                    start(odd, gram)

                    @pl.when(with_gram == gram)
                    def _():
                        def tile(k):
                            n = 2 - odd + 2 * k
                            body(b, c, base + n * H, v0 + 2 * n * S, 4, gram, False)
                        loop(0, (m + odd) // 2 - 1, tile)
                rs_wait(i + 2)
                rs_sum(i + 2)
                wsend[c] = (wacc[0] + wprod(b - 1, NL - 2 * K, 2)) + (wacc[1] + wprod(b - 1, NL - K, 3))
                y_send(i + 2)
                w_send(c)

        for tiles in range(FLAT, M + 1):
            @pl.when(m == tiles)
            def _():
                for gram in (True, False):
                    start(tiles, gram)

                @pl.when(jnp.logical_not(begin))
                def _():
                    w_send(before)
                rs_wait(i + 2)
                rs_sum(i + 2)
                half(b, c, tiles, v0, True, None, False)
                y_send(i + 2)

        @pl.when(c == 3)
        def _():
            @pl.when(jnp.logical_and(own(b - 2), b >= 2))
            def _():
                g_fin(b - 2)

            @pl.when(with_gram)
            def _():
                g_start(q3)

            @pl.when(q3 >= 2)
            def _():
                release(q3)

    loop(0, 4 * B0, slot)
    if FLAT <= M:
        wsend[3] = (wacc[0] + wprod(0, NL - 2 * K, 2)) + (wacc[1] + wprod(0, NL - K, 3))
        w_send(3)

    def out_copy(c):
        return pltpu.make_async_copy(xT.at[chunk(c), :], out_hbm.at[chunk(c), :], o_sem.at[c])

    def end_slot(c):
        @pl.when(c < 2)
        def _():
            j = 4 * B0 + c + 2
            rs_wait(j)
            rs_sum(j)
            y_send(j)
        y_take(c)

        def tile(t):
            upd(0, c, t * 2 * H, None, 2 * H)
        loop(0, M // 2, tile)
        out_copy(c).start()
    loop(0, 4, end_slot)

    for c in range(4):
        out_copy(c).wait()

    def z_sent(k):
        for p in CHIPS3:
            z_remote(k, p).wait_send()
    loop(0, min(4, ZE), z_sent)
    for p in CHIPS3:
        x_remote(p).wait_send()
        for k in range(TAIL):
            e_remote(k, k // 2, p).wait_send()
    for k in range(TAIL):
        f_remote(k).wait_send()
        for p in CHIPS4:
            d_remote(k, k // 2, p).wait_send()
    sent(1)
    sent(0)


def solution(mesh):
    def local_apply(v_loc, t_loc, z_loc):
        NL, half = v_loc.shape
        NB = half // 128
        H = min(512, NL // 8)
        tiles = NL // H
        z_t = z_loc.T
        any_ = pl.BlockSpec(memory_space=pl.ANY)
        dma = pltpu.SemaphoreType.DMA
        vmem = pltpu.VMEM
        x_t = pl.pallas_call(
            functools.partial(kernel, H, NB),
            out_shape=jax.ShapeDtypeStruct((4 * C, NL), F32),
            in_specs=[any_] * 3,
            out_specs=any_,
            scratch_shapes=[
                vmem((4 * C, NL), F32),
                vmem((2, 2, NL, 128), F32),
                vmem((4, 3, NL, B), BF16),
                vmem((4, 2, 128, 128), F32),
                vmem((2, 3, B, B), BF16),
                vmem((3 * C, B), BF16),
                vmem((4, 3 * C, H // 2), BF16),
                vmem((2, C, B), F32),
                vmem((5, C, B), F32),
                vmem((4, 3, SH, B), F32),
                vmem((4, SH, B), F32),
                vmem((4, C, B), F32),
                vmem((128, 128), F32),
                vmem((128, 128), F32),
                vmem((3, SH, 128), F32),
                vmem((SH, 128), F32),
                vmem((128, 128), F32),
                vmem((2, 128, 128), F32),
                vmem((2, 128, 128), F32),
                vmem((TAIL, 2, 4, 64 * TAIL, 128), F32),
                vmem((TAIL, 2, 128, 128), F32),
                vmem((C, 4 * 64 * TAIL), F32),
                vmem((4, 3, C, 128), F32),
                dma((NL // 128, 3)), dma((NL // 128, 3)), dma((NL // 128,)), dma((4, 3)),
                *[dma((2, tiles))] * 3, *[dma((4,))] * 3,
                *[dma((4, 3))] * 5, dma((2,)), dma((2,)), dma((4,)),
                dma((2, TAIL, 3)), dma((2, TAIL, 5)), dma((3, max(TAIL, 4))), dma((2, 3)),
                pltpu.SemaphoreType.REGULAR,
            ],
            compiler_params=pltpu.CompilerParams(
                collective_id=0, has_side_effects=True, vmem_limit_bytes=62 * 1024 * 1024),
            name='back_transform',
        )(t_loc, v_loc, z_t)
        return x_t.T

    return jax.shard_map(local_apply, mesh=mesh,
                         in_specs=(P('row', 'col'), P('col', None, None), P(None, ('col', 'row'))),
                         out_specs=P('row', 'col'), check_vma=False)
```
